256 devices in a mesh: obs: 32 (over y, z), chan: 8 (over x, core).
Axes of the slice: x: 4, y: 4, z: 8, core: 2. Of those that a mesh axis runs over, the one named last changes fastest.
Arguments:
- jacobian: bfloat16 [8192, 256, 137], P('obs', 'chan'), may hold values from -0.5 to 0.5
- departures: float32 [256, 8192], P('chan', 'obs'), may hold values from -6 to 6
- obs_weights: float32 [256, 8192], P('chan', 'obs'), may hold values from 0.25 to 4
- column_count: int32 [32], P('obs'), may hold values from 1 to 256, as said below
- grid_block: int32 [64], P('obs'), may hold values from 0 to 63, as said below
- sqrt_cov: float32 [137, 137], replicated, may hold values from -0.5 to 0.5
Outputs:
- increment: float32 [8192, 137], P('obs')
- residual: float32 [8192, 137], P('obs')
The draws below stay inside these ranges and needn't reach their ends.
Inputs may be any that keep to these rules, and one draw needn't show every extreme that they name: The first column_count of a device's 256 column slots are observed; some device has all 256 observed in every draw. `grid_block`: the owner of grid block g is index g // 2 of obs. The 2 blocks of one device match blocks of 2 different owners; in every draw some owner has a block matched by each device (every device matches one of that owner's blocks), and some device matches that owner's last block.
All inputs are finite; a program needn't handle non-finite values.
Results may differ from the reference program's by a relative error of at most 0.02.
Values may be sent and summed in bfloat16 or wider, within the bound.
A program may use at most 64 MiB of HBM per device.

```python
import math
import jax
import jax.numpy as jnp
from jax import lax

L = 137
BLOCK = 128
ITERS = 5
OBS_BLK = 2
GRID_BLK = 2
CHANNELS = 256
COLS = 8192
N_OBS = 32


def draw_column_count(key, part):
    span = OBS_BLK * BLOCK
    drawn = jax.random.randint(jax.random.fold_in(key, 11), (N_OBS,), 0, span + 1)
    counts = jnp.maximum(drawn * drawn // span, 1)
    fullest = jax.random.randint(jax.random.fold_in(key, 12), (), 0, N_OBS)
    counts = jnp.where(jnp.arange(N_OBS) == fullest, span, counts)
    return counts.astype(jnp.int32)


def draw_grid_block(key, part):
    common = jax.random.randint(jax.random.fold_in(key, 21), (), 0, N_OBS)
    scores = jax.random.randint(jax.random.fold_in(key, 22), (N_OBS, N_OBS), 0, 1048576)
    scores = scores * N_OBS + jnp.arange(N_OBS)[None, :]
    scores = jnp.where(jnp.arange(N_OBS)[None, :] == common, -1, scores)
    owners = jnp.argsort(scores, axis=1, stable=True)[:, :OBS_BLK]
    places = jax.random.randint(jax.random.fold_in(key, 23), (N_OBS, OBS_BLK), 0, GRID_BLK)
    chosen = jax.random.randint(jax.random.fold_in(key, 24), (), 0, N_OBS)
    rows = jnp.arange(N_OBS)[:, None]
    slots = jnp.arange(OBS_BLK)[None, :]
    places = jnp.where((rows == chosen) & (slots == 0), GRID_BLK - 1, places)
    return (owners * GRID_BLK + places).reshape(-1).astype(jnp.int32)


def steps_of(rng, extent, cuts, least, high):
    factor_of = 1.0
    for dim, blocks in cuts:
        draws = jax.random.uniform(jax.random.fold_in(jax.random.fold_in(rng, 6), dim), (blocks,), jnp.float32, least / len(cuts), high / len(cuts))
        factor_of = factor_of * jnp.repeat(jnp.exp(draws), extent[dim] // blocks).reshape((-1,) + (1,) * (len(extent) - 1 - dim))
    return factor_of


def scatter_about(stream_key, shape, scale, bound, cuts=(), held_as=jnp.bfloat16):
    result = scale * jax.random.normal(stream_key, shape, jnp.float32)
    if cuts:
        result = result * steps_of(stream_key, shape, cuts, -0.22, 0.18)
    return jnp.clip(result, -bound, bound).astype(held_as)


def setup_inputs(seed: int = 0) -> dict:
    arg_keys = jax.random.split(jax.random.key(seed), 7)
    jacobian = scatter_about(arg_keys[0], (COLS, CHANNELS, L), L ** -0.5, 0.5, ((0, 32), (1, 8)))
    departures = scatter_about(arg_keys[1], (CHANNELS, COLS), 1.0, 6.0, ((0, 8), (1, 32)), jnp.float32)
    obs_weights = jnp.clip(jnp.exp(math.log(4.0) - 2.7725887 * jax.random.uniform(arg_keys[2], (CHANNELS, COLS), jnp.float32) ** steps_of(arg_keys[2], (CHANNELS, COLS), ((0, 8), (1, 32)), -0.2, 0.2)), 0.25, 4.0)
    column_count = draw_column_count(jax.random.fold_in(arg_keys[6], 71), 0)
    grid_block = draw_grid_block(jax.random.fold_in(arg_keys[6], 71), 0)
    sqrt_cov = scatter_about(arg_keys[5], (L, L), L ** -0.5, 0.5, (), jnp.float32)
    return {"jacobian": jacobian, "departures": departures, "obs_weights": obs_weights, "column_count": column_count, "grid_block": grid_block, "sqrt_cov": sqrt_cov}


def source_block(operands):
    jac_part, weight_part, mask_part, depart_part = operands
    kernel = jac_part.astype(jnp.float32)
    scaled = (mask_part[:, None] * weight_part * depart_part).astype(jnp.bfloat16)
    scaled = lax.optimization_barrier(scaled).astype(jnp.float32)
    return jnp.einsum('cnl,cn->cl', kernel, scaled, precision=lax.Precision.HIGHEST)

def normal_block(operands):
    jac_part, weight_part, mask_part, field_part = operands
    kernel = jac_part.astype(jnp.float32)
    predicted = jnp.einsum('cnl,cl->cn', kernel, field_part.astype(jnp.float32), precision=lax.Precision.HIGHEST)
    scaled = (mask_part[:, None] * weight_part * predicted).astype(jnp.bfloat16)
    scaled = lax.optimization_barrier(scaled).astype(jnp.float32)
    return jnp.einsum('cnl,cn->cl', kernel, scaled, precision=lax.Precision.HIGHEST)

def reference(jacobian, departures, obs_weights, column_count, grid_block, sqrt_cov):
    columns_all = jacobian.shape[0]
    per_device = OBS_BLK * BLOCK
    position = jnp.arange(columns_all, dtype=jnp.int32)
    observed = (position % per_device < column_count[position // per_device]).astype(jnp.float32)
    block_total = columns_all // BLOCK
    jac_blocks = jacobian.reshape(block_total, BLOCK, CHANNELS, L)
    weight_blocks = obs_weights.T.reshape(block_total, BLOCK, CHANNELS)
    depart_blocks = departures.T.reshape(block_total, BLOCK, CHANNELS)
    mask_blocks = observed.reshape(block_total, BLOCK)
    grid_total = GRID_BLK * N_OBS

    def collect(terms):
        summed = jnp.zeros((grid_total, BLOCK, L), jnp.float32).at[grid_block].add(terms)
        return summed.reshape(grid_total * BLOCK, L)

    def spread(field):
        return jnp.dot(field, sqrt_cov, precision=lax.Precision.HIGHEST)

    def spread_back(field):
        return jnp.dot(field, sqrt_cov.T, precision=lax.Precision.HIGHEST)

    def normal(direction):
        rounded = lax.optimization_barrier(spread(direction).astype(jnp.bfloat16))
        fields = rounded.reshape(grid_total, BLOCK, L)[grid_block]
        terms = lax.map(normal_block, (jac_blocks, weight_blocks, mask_blocks, fields))
        return direction + spread_back(collect(terms))
    source_terms = lax.map(source_block, (jac_blocks, weight_blocks, mask_blocks, depart_blocks))
    residual = spread_back(collect(source_terms))
    control = jnp.zeros_like(residual)
    direction = residual
    norm_now = jnp.sum(residual * residual)
    for iteration in range(ITERS):
        image = normal(direction)
        step_length = norm_now / jnp.sum(direction * image)
        control = control + step_length * direction
        residual = residual - step_length * image
        norm_next = jnp.sum(residual * residual)
        direction = residual + norm_next / norm_now * direction
        norm_now = norm_next
    return (spread(control), residual)
```

```python
import jax
import jax.numpy as jnp
from jax import lax
from jax.experimental import pallas as pl
from jax.experimental.pallas import tpu as pltpu
from jax.sharding import Mesh
from jax.sharding import PartitionSpec as P

ITERS = 5
L = 137
NY, NZ, NX, NC = 4, 8, 4, 2
NCH = NX * NC
NM = NY * NCH
LH = 35
CHUNKS = 5
PER = LH // CHUNKS
WIDE = LH * 128
ID_LANE = 200
OBS = ("obs_0", "obs_1")
CHAN = ("chan_0", "chan_1")
MESH = pl.DeviceIdType.MESH
F32 = jnp.float32
BF16 = jnp.bfloat16


def iota(shape, dim):
    return lax.broadcasted_iota(jnp.int32, shape, dim)


def dot(a, b):
    return jnp.dot(a, b, preferred_element_type=F32)


def dot_t(a, b):
    return lax.dot_general(a, b, (((1,), (1,)), ((), ())), preferred_element_type=F32)


def halves(v):
    hi = v.astype(BF16)
    return hi, (v - hi.astype(F32)).astype(BF16)


def lanes(q):
    return pl.ds(q * 128, 128)


def kernel(
    cnt_ref, gb_ref, jt_ref, w_ref, d_ref, s_ref,
    inc_ref, res_ref,
    sb, jr, mw, sd, fx, sv, ts, sh, sl, perm, eye, own, pick, ids,
    r, p, s, x, mz, sx, sz, out, got,
    js, jq, zs, zq, xs, xq, vs, vq, ys, yq, os, oq,
):
    my_y = lax.axis_index("obs_0")
    my_z = lax.axis_index("obs_1")
    my_x = lax.axis_index("chan_0")
    my_c = lax.axis_index("chan_1")
    my_m = my_y * NCH + my_x * NC + my_c

    def plane_peer(m):
        return (m // NCH, my_z, (m % NCH) // NC, m % NC)

    def ring_peer(z):
        return (my_y, z, my_x, my_c)

    barrier = pltpu.get_barrier_semaphore()

    def greet_plane(t, carry):
        pl.semaphore_signal(barrier, inc=1, device_id=plane_peer((my_m + t) % NM), device_id_type=MESH)
        return carry

    def greet_ring(t, carry):
        pl.semaphore_signal(barrier, inc=1, device_id=ring_peer((my_z + t) % NZ), device_id_type=MESH)
        return carry

    lax.fori_loop(1, NM, greet_plane, 0)
    lax.fori_loop(1, NZ, greet_ring, 0)

    row = iota((256, 256), 0)
    col = iota((256, 256), 1)
    perm[...] = jnp.where((row % 8) // 4 * 128 + (row // 8) * 4 + row % 4 == col, 1.0, 0.0).astype(BF16)
    eye[...] = jnp.where(row == col, 1.0, 0.0).astype(BF16)
    sh[...] = jnp.zeros_like(sh)
    sl[...] = jnp.zeros_like(sl)
    root_hi, root_lo = halves(s_ref[...])
    sh[0:L, 0:L] = root_hi
    sl[0:L, 0:L] = root_lo
    r4 = iota((8, 128), 0)
    ids[my_y] = jnp.where(r4 < 4, gb_ref[0], gb_ref[1]).astype(F32)
    mask = jnp.where(iota((32, 256), 1) < cnt_ref[0], 1.0, 0.0)
    weight = mask * w_ref[...]
    weight_hi, weight_lo = halves(weight)
    scaled_d = (weight * d_ref[...]).astype(BF16)

    pl.semaphore_wait(barrier, NM - 1 + NZ - 1)

    def id_copy(t):
        peer = (my_y + t) % NY
        return pltpu.make_async_remote_copy(
            src_ref=ids.at[my_y], dst_ref=ids.at[my_y], send_sem=ys.at[t], recv_sem=yq.at[my_y],
            device_id=(peer, my_z, my_x, my_c), device_id_type=MESH)

    def id_arrival(t):
        peer = (my_y + t) % NY
        return pltpu.make_async_remote_copy(
            src_ref=ids.at[peer], dst_ref=ids.at[peer], send_sem=ys.at[t], recv_sem=yq.at[peer],
            device_id=(peer, my_z, my_x, my_c), device_id_type=MESH)

    for t in range(1, NY):
        id_copy(t).start()

    for q in range(CHUNKS):
        def turn(i, carry):
            h = q * PER + i
            block = jt_ref[pl.ds(4 * h, 4)].reshape(128, 256)
            turned = dot_t(perm[...], block).astype(BF16)
            sb[:, :, pl.ds(pl.multiple_of(h * 128, 128), 128)] = turned.reshape(NM, 8, 128)
            return carry

        if q < CHUNKS - 1:
            lax.fori_loop(0, PER, turn, 0)
        else:
            lax.fori_loop(0, PER - 1, turn, 0)
            block = jnp.concatenate([jt_ref[L - 1], weight_hi, weight_lo, scaled_d], axis=0)
            turned = dot_t(perm[...], block).astype(BF16)
            sb[:, :, lanes(LH - 1)] = turned.reshape(NM, 8, 128)

        def send(t, carry):
            m = (my_m + t) % NM
            part = pl.ds(q * PER * 128, PER * 128)
            pltpu.make_async_remote_copy(
                src_ref=sb.at[m, :, part], dst_ref=jr.at[my_m, :, part],
                send_sem=js.at[m], recv_sem=jq.at[my_m],
                device_id=plane_peer(m), device_id_type=MESH).start()
            return carry

        lax.fori_loop(1, NM, send, 0)

    jr[my_m] = sb[my_m]

    for t in range(1, NY):
        id_arrival(t).wait()

    def j_arrival(m):
        return pltpu.make_async_remote_copy(
            src_ref=sb.at[m], dst_ref=jr.at[m], send_sem=js.at[m], recv_sem=jq.at[m],
            device_id=plane_peer(m), device_id_type=MESH)

    def arrive(t, carry):
        j_arrival((my_m + t) % NM).wait()
        return carry

    lax.fori_loop(1, NM, arrive, 0)

    lane = iota((8, 128), 1)
    lane2 = iota((8, 256), 1)
    row2 = iota((8, 256), 0)

    def across(v):
        v = v + pltpu.roll(v, 64, 1)
        return v + pltpu.roll(v, 32, 1)

    def unpack(m, carry):
        extra = jr[m, :, lanes(LH - 1)].astype(F32)
        mw[m] = across(jnp.where((lane >= 32) & (lane < 96), extra, 0.0))
        sd[m] = across(jnp.where(lane >= 96, extra, 0.0))
        return carry

    lax.fori_loop(0, NM, unpack, 0)

    for y in range(NY):
        ident = ids[y][:, 0:1]
        own[pl.ds(8 * y, 8), :] = jnp.where(
            (ident.astype(jnp.int32) == lane2 // 4) & (row2 % 4 == lane2 % 4), 1.0, 0.0)

    def ring_copy(buf, send_sem, recv_sem, slot, t):
        return pltpu.make_async_remote_copy(
            src_ref=buf.at[slot, my_z], dst_ref=buf.at[slot, my_z],
            send_sem=send_sem.at[slot, t], recv_sem=recv_sem.at[slot, my_z],
            device_id=ring_peer((my_z + t) % NZ), device_id_type=MESH)

    def ring_arrival(buf, send_sem, recv_sem, slot, t):
        z = (my_z + t) % NZ
        return pltpu.make_async_remote_copy(
            src_ref=buf.at[slot, z], dst_ref=buf.at[slot, z],
            send_sem=send_sem.at[slot, t], recv_sem=recv_sem.at[slot, z],
            device_id=ring_peer(z), device_id_type=MESH)

    FAR_FIRST = (4, 3, 5, 2, 6, 1, 7)

    def terms(factor, slot):
        def group(y, carry):
            acc = []
            for h in range(LH):
                total = None
                for c in range(NCH):
                    m = y * NCH + c
                    prod = jr[m, :, lanes(h)].astype(F32) * factor[m]
                    total = prod if total is None else total + prod
                acc.append(total)
            stacked = jnp.concatenate(acc, axis=0)
            hi, lo = halves(stacked)
            spot = jnp.where(iota((128, 128), 0) // 32 == iota((128, 128), 1) % 4, 1.0, 0.0).astype(BF16)
            sums = dot(hi, spot) + dot(lo, spot)
            first = jnp.zeros((8, 128), F32)
            second = jnp.zeros((8, 128), F32)
            for h in range(LH):
                piece = jnp.where(lane // 4 == h % 32, sums[8 * h: 8 * h + 8], 0.0)
                if h < 32:
                    first = first + piece
                else:
                    second = second + piece
            ts[y, :, 0:128] = first
            ts[y, :, 128:256] = second
            return carry

        lax.fori_loop(0, NY, group, 0)
        hi, lo = halves(ts[...].reshape(32, 256))
        back = dot_t(hi, sh[...]) + dot_t(lo, sh[...]) + dot_t(hi, sl[...])
        back = back.reshape(NY, 8, 256)
        back = jnp.where(iota((NY, 8, 256), 2) == ID_LANE, jnp.concatenate([ids[...]] * 2, axis=2), back)
        mz[slot, my_z] = back.reshape(32, 256).astype(BF16)
        for t in FAR_FIRST:
            ring_copy(mz, zs, zq, slot, t).start()

    def ring_wait(buf, send_sem, recv_sem, slot):
        for t in range(1, NZ):
            ring_arrival(buf, send_sem, recv_sem, slot, t).wait()

    terms(sd, 0)
    ring_wait(mz, zs, zq, 0)
    every = mz[0].reshape(256, 256)
    ident = every[:, ID_LANE: ID_LANE + 1].astype(F32).astype(jnp.int32)
    match = jnp.where((ident == col // 4) & (row % 4 == col % 4), 1.0, 0.0).astype(BF16)
    pick[...] = dot_t(eye[...], match).astype(BF16)
    body = jnp.where(col < L, dot(pick[...], every), 0.0)
    r[...] = body
    p[...] = jnp.zeros_like(body)
    s[...] = jnp.zeros_like(body)
    x[...] = jnp.zeros_like(body)

    def plane_copy(slot, t):
        m = (my_m + t) % NM
        return pltpu.make_async_remote_copy(
            src_ref=sx.at[slot, my_m], dst_ref=sx.at[slot, my_m],
            send_sem=xs.at[slot, m], recv_sem=xq.at[slot, my_m],
            device_id=plane_peer(m), device_id_type=MESH)

    def plane_arrival(slot, t):
        m = (my_m + t) % NM
        return pltpu.make_async_remote_copy(
            src_ref=sx.at[slot, m], dst_ref=sx.at[slot, m],
            send_sem=xs.at[slot, m], recv_sem=xq.at[slot, m],
            device_id=plane_peer(m), device_id_type=MESH)

    def iteration(i, carry):
        norm_old, step_old = carry
        slot = (i + 1) % 2
        res = r[...]
        hi, lo = halves(res)
        choose = own[...].astype(BF16)
        near_hi = dot(choose, hi).astype(BF16)
        near_lo = dot(choose, lo).astype(BF16)
        field = dot(near_hi, sh[...]) + dot(near_lo, sh[...]) + dot(near_hi, sl[...])
        field = field.astype(BF16).astype(F32).reshape(NY, 8, 256)
        ts[...] = field
        squares = jnp.sum(res * res, axis=0, keepdims=True)
        squares = squares[:, 0:128] + squares[:, 128:256]

        def predict(y, carry):
            for h in range(LH):
                base = ts[y, :, 0:128] if h < 32 else ts[y, :, 128:256]
                fx[:, lanes(h)] = jnp.take_along_axis(base, 4 * (h % 32) + lane // 32, axis=1)
            for c in range(NCH):
                m = y * NCH + c
                total = jnp.zeros((8, 128), F32)
                for h in range(LH):
                    total = total + jr[m, :, lanes(h)].astype(F32) * fx[:, lanes(h)]
                total = across(total)
                scaled = mw[m] * total
                sv[m] = scaled
                carry = carry + scaled * total
            return carry

        bends = lax.fori_loop(0, NY, predict, jnp.zeros((8, 128), F32))
        bends = jnp.sum(bends, axis=0, keepdims=True) * 0.25
        lane1 = iota((1, 128), 1)
        sx[slot, my_m] = jnp.where(
            lane1 < 64, squares + pltpu.roll(squares, 64, 1), bends + pltpu.roll(bends, 64, 1))

        def start(t, carry):
            plane_copy(slot, t).start()
            return carry

        lax.fori_loop(1, NM, start, 0)
        terms(sv, slot)

        def finish(t, carry):
            plane_arrival(slot, t).wait()
            return carry

        lax.fori_loop(1, NM, finish, 0)
        plane = jnp.sum(sx[slot], axis=0)
        sz[slot, my_z] = plane
        for t in FAR_FIRST:
            ring_copy(sz, vs, vq, slot, t).start()
        ring_wait(mz, zs, zq, slot)
        image = res + jnp.where(col < L, dot(pick[...], mz[slot].reshape(256, 256)), 0.0)
        ring_wait(sz, vs, vq, slot)
        ring = jnp.sum(sz[slot], axis=0)
        norm = jnp.sum(jnp.where(lane1 < 64, plane, 0.0), axis=1, keepdims=True)
        bend = norm + jnp.sum(jnp.where(lane1 >= 64, ring, 0.0), axis=1, keepdims=True)
        first = i == 0
        ratio = jnp.where(first, 0.0, norm / norm_old)
        step = norm / (bend - jnp.where(first, 0.0, ratio * norm / step_old))
        turned = image + ratio * s[...]
        s[...] = turned
        ahead = res + ratio * p[...]
        p[...] = ahead
        x[...] = x[...] + step * ahead
        r[...] = res - step * turned
        return norm, step

    one = jnp.ones((1, 1), F32)
    lax.fori_loop(0, ITERS, iteration, (one, one))

    hi, lo = halves(x[...])
    grown = dot(hi, sh[...]) + dot(lo, sh[...]) + dot(hi, sl[...])
    out[:, 0:8, :] = grown.astype(BF16).reshape(NM, 8, 256)
    out[:, 8:16, :] = r[...].astype(BF16).reshape(NM, 8, 256)

    def give(t, carry):
        m = (my_m + t) % NM
        pltpu.make_async_remote_copy(
            src_ref=out.at[m // NCH * NZ + my_z], dst_ref=got.at[my_m],
            send_sem=os.at[m], recv_sem=oq.at[my_m],
            device_id=plane_peer(m), device_id_type=MESH).start()
        return carry

    lax.fori_loop(1, NM, give, 0)
    got[my_m] = out[my_y * NZ + my_z]

    def take(t, carry):
        m = (my_m + t) % NM
        pltpu.make_async_remote_copy(
            src_ref=out.at[m // NCH * NZ + my_z], dst_ref=got.at[m],
            send_sem=os.at[m], recv_sem=oq.at[m],
            device_id=plane_peer(m), device_id_type=MESH).wait()
        return carry

    lax.fori_loop(1, NM, take, 0)
    for k, ref in ((0, inc_ref), (1, res_ref)):
        rows = got[:, 8 * k: 8 * k + 8, :].reshape(256, 256)
        flat = dot_t(eye[...], rows).astype(BF16)
        ref[...] = dot(flat, perm[...])[0:L]


def per_device(jacobian, departures, obs_weights, column_count, grid_block, sqrt_cov):
    jt = jnp.transpose(jacobian, (2, 1, 0))
    vmem = pl.BlockSpec(memory_space=pltpu.VMEM)
    smem = pl.BlockSpec(memory_space=pltpu.SMEM)
    dma = pltpu.SemaphoreType.DMA
    inc, res = pl.pallas_call(
        kernel,
        out_shape=(jax.ShapeDtypeStruct((L, 256), F32),) * 2,
        in_specs=[smem, smem, vmem, vmem, vmem, vmem],
        out_specs=(vmem, vmem),
        scratch_shapes=[
            pltpu.VMEM((NM, 8, WIDE), BF16),
            pltpu.VMEM((NM, 8, WIDE), BF16),
            pltpu.VMEM((NM, 8, 128), F32),
            pltpu.VMEM((NM, 8, 128), F32),
            pltpu.VMEM((8, WIDE), F32),
            pltpu.VMEM((NM, 8, 128), F32),
            pltpu.VMEM((NY, 8, 256), F32),
            pltpu.VMEM((256, 256), BF16),
            pltpu.VMEM((256, 256), BF16),
            pltpu.VMEM((256, 256), BF16),
            pltpu.VMEM((256, 256), BF16),
            pltpu.VMEM((32, 256), F32),
            pltpu.VMEM((256, 256), BF16),
            pltpu.VMEM((NY, 8, 128), F32),
            pltpu.VMEM((256, 256), F32),
            pltpu.VMEM((256, 256), F32),
            pltpu.VMEM((256, 256), F32),
            pltpu.VMEM((256, 256), F32),
            pltpu.VMEM((2, NZ, 32, 256), BF16),
            pltpu.VMEM((2, NM, 1, 128), F32),
            pltpu.VMEM((2, NZ, 1, 128), F32),
            pltpu.VMEM((NM, 16, 256), BF16),
            pltpu.VMEM((NM, 16, 256), BF16),
            dma((NM,)), dma((NM,)),
            dma((2, NZ)), dma((2, NZ)),
            dma((2, NM)), dma((2, NM)),
            dma((2, NZ)), dma((2, NZ)),
            dma((NY,)), dma((NY,)),
            dma((NM,)), dma((NM,)),
        ],
        compiler_params=pltpu.CompilerParams(
            collective_id=0, has_side_effects=True, vmem_limit_bytes=50 * 1024 * 1024),
        name="cg",
    )(column_count, grid_block, jt, obs_weights, departures, sqrt_cov)
    return inc.T, res.T


def solution(mesh):
    split = Mesh(mesh.devices.reshape(NY, NZ, NX, NC), ("obs_0", "obs_1", "chan_0", "chan_1"))
    return jax.shard_map(
        per_device,
        mesh=split,
        in_specs=(P(OBS, CHAN, None), P(CHAN, OBS), P(CHAN, OBS), P(OBS), P(OBS), P()),
        out_specs=(P(OBS, None), P(OBS, None)),
        check_vma=False,
    )
```

```python
import jax
import jax.numpy as jnp
from jax import lax
from jax.experimental import pallas as pl
from jax.experimental.pallas import tpu as pltpu
from jax.sharding import Mesh
from jax.sharding import PartitionSpec as P

ITERS = 5
L = 137
NY, NZ, NX, NC = 4, 8, 4, 2
NCH = NX * NC
NM = NY * NCH
LH = 35
CHUNKS = 5
PER = LH // CHUNKS
WIDE = LH * 128
ID_LANE = 16
OBS = ("obs_0", "obs_1")
CHAN = ("chan_0", "chan_1")
MESH = pl.DeviceIdType.MESH
F32 = jnp.float32
BF16 = jnp.bfloat16


def iota(shape, dim):
    return lax.broadcasted_iota(jnp.int32, shape, dim)


def dot(a, b):
    return jnp.dot(a, b, preferred_element_type=F32)


def dot_t(a, b):
    return lax.dot_general(a, b, (((1,), (1,)), ((), ())), preferred_element_type=F32)


def halves(v):
    hi = v.astype(BF16)
    return hi, (v - hi.astype(F32)).astype(BF16)


def lanes(q):
    return pl.ds(q * 128, 128)


def kernel(
    cnt_hbm, gb_hbm, jt_hbm, w_hbm, d_hbm, s_hbm,
    inc_ref, res_ref,
    cnt_ref, gb_ref, jv, w_ref, d_ref, s_ref,
    sb, jr, mw, fx, sv, ts, sh, sl, perm, eye, spot, own, pick, ids, tt, so, sr, cm,
    r, p, s, x, w, v, mz, sx, out, got,
    fs, js, jq, as_, aq, zs, zq, xs, xq, ys, yq, os, oq,
):
    my_y = lax.axis_index("obs_0")
    my_z = lax.axis_index("obs_1")
    my_x = lax.axis_index("chan_0")
    my_c = lax.axis_index("chan_1")
    my_m = my_y * NCH + my_x * NC + my_c

    fetches = [
        pltpu.make_async_copy(a, b, fs.at[k])
        for k, (a, b) in enumerate((
            (w_hbm, w_ref), (d_hbm, d_ref), (cnt_hbm, cnt_ref), (gb_hbm, gb_ref), (s_hbm, s_ref)))
    ]
    blocks = []
    for q in range(CHUNKS):
        first, last = 4 * PER * q, min(4 * PER * (q + 1), L)
        blocks.append(pltpu.make_async_copy(
            jt_hbm.at[first:last], jv.at[first:last], fs.at[len(fetches) + q]))
    for copy in (blocks[0], *fetches, *blocks[1:]):
        copy.start()

    def plane_peer(m):
        return (m // NCH, my_z, (m % NCH) // NC, m % NC)

    def ring_peer(z):
        return (my_y, z, my_x, my_c)

    barrier = pltpu.get_barrier_semaphore()

    def greet_plane(t, carry):
        pl.semaphore_signal(barrier, inc=1, device_id=plane_peer((my_m + t) % NM), device_id_type=MESH)
        return carry

    def greet_ring(t, carry):
        pl.semaphore_signal(barrier, inc=1, device_id=ring_peer((my_z + t) % NZ), device_id_type=MESH)
        return carry

    lax.fori_loop(1, NM, greet_plane, 0)
    lax.fori_loop(1, NZ, greet_ring, 0)

    row = iota((256, 256), 0)
    col = iota((256, 256), 1)
    lane = iota((8, 128), 1)
    lane1 = iota((1, 128), 1)
    perm[...] = jnp.where(
        ((row & 4) << 5) + ((row >> 3) << 2) + (row & 3) == col, 1.0, 0.0).astype(BF16)
    jv[L:144] = jnp.zeros((144 - L, 32, 256), BF16)

    def turn(h, carry):
        block = jv[pl.ds(4 * h, 4)].reshape(128, 256)
        turned = dot_t(perm[...], block).astype(BF16)
        sb[:, :, pl.ds(pl.multiple_of(h * 128, 128), 128)] = turned.reshape(NM, 8, 128)
        return carry

    def send_chunk(q):
        def send(t, carry):
            m = (my_m + t) % NM
            part = pl.ds(q * PER * 128, PER * 128)
            pltpu.make_async_remote_copy(
                src_ref=sb.at[m, :, part], dst_ref=jr.at[my_m, :, part],
                send_sem=js.at[m], recv_sem=jq.at[my_m],
                device_id=plane_peer(m), device_id_type=MESH).start()
            return carry

        lax.fori_loop(1, NM, send, 0)

    blocks[0].wait()
    lax.fori_loop(0, PER, turn, 0, unroll=True)
    pl.semaphore_wait(barrier, NM - 1 + NZ - 1)
    send_chunk(0)

    for copy in fetches:
        copy.wait()
    sh[...] = jnp.zeros_like(sh)
    sl[...] = jnp.zeros_like(sl)
    root_hi, root_lo = halves(s_ref[...])
    sh[0:L, 0:L] = root_hi
    sl[0:L, 0:L] = root_lo
    r4 = iota((8, 128), 0)
    ids[my_y] = jnp.where(r4 < 4, gb_ref[0], gb_ref[1]).astype(F32)

    def id_copy(t, arriving):
        peer = (my_y + t) % NY
        at = peer if arriving else my_y
        return pltpu.make_async_remote_copy(
            src_ref=ids.at[at], dst_ref=ids.at[at], send_sem=ys.at[t], recv_sem=yq.at[at],
            device_id=(peer, my_z, my_x, my_c), device_id_type=MESH)

    for t in range(1, NY):
        id_copy(t, False).start()

    mask = jnp.where(iota((32, 256), 1) < cnt_ref[0], 1.0, 0.0)
    weight = mask * w_ref[...]
    weight_hi, weight_lo = halves(weight)
    scaled_d = (weight * d_ref[...]).astype(BF16)
    d_ref[...] = scaled_d.astype(F32)

    for copy in blocks[1:]:
        copy.wait()

    def gather_source(g, carry):
        part = jv[pl.ds(8 * g, 8)].astype(F32) * d_ref[...][None]
        tt[pl.ds(pl.multiple_of(8 * g, 8), 8), :] = jnp.sum(part, axis=1)
        return carry

    lax.fori_loop(0, 18, gather_source, 0, unroll=2)
    hi, lo = halves(tt[...])
    flat = dot_t(perm[...], hi) + dot_t(perm[...], lo)
    hi, lo = halves(flat)
    front = sh[:, 0:144]
    flat = dot_t(hi, front) + dot_t(lo, front) + dot_t(hi, sl[:, 0:144])
    so[...] = flat.astype(BF16).reshape(NM, 8, 256)

    def source_copy(t, arriving):
        m = (my_m + t) % NM
        return pltpu.make_async_remote_copy(
            src_ref=so.at[m], dst_ref=sr.at[m if arriving else my_m],
            send_sem=as_.at[m], recv_sem=aq.at[m if arriving else my_m],
            device_id=plane_peer(m), device_id_type=MESH)

    def source_send(t, carry):
        source_copy(t, False).start()
        return carry

    lax.fori_loop(1, NM, source_send, 0)
    sr[my_m] = so[my_m]

    for q in range(1, CHUNKS):
        if q < CHUNKS - 1:
            lax.fori_loop(q * PER, (q + 1) * PER, turn, 0, unroll=True)
        else:
            lax.fori_loop(q * PER, (q + 1) * PER - 1, turn, 0, unroll=True)
            block = jnp.concatenate([jv[L - 1], weight_hi, weight_lo, jnp.zeros_like(weight_hi)], axis=0)
            turned = dot_t(perm[...], block).astype(BF16)
            sb[:, :, lanes(LH - 1)] = turned.reshape(NM, 8, 128)
        send_chunk(q)
    jr[my_m] = sb[my_m]

    eye[...] = jnp.where(row == col, 1.0, 0.0).astype(BF16)
    spot[...] = jnp.where(
        iota((128, 128), 0) >> 5 == (iota((128, 128), 1) & 3), 1.0, 0.0).astype(BF16)
    for t in range(1, NY):
        id_copy(t, True).wait()
    row2 = iota((8, 256), 0)
    lane2 = iota((8, 256), 1)
    for y in range(NY):
        ident = ids[y][:, 0:1].astype(jnp.int32)
        own[pl.ds(8 * y, 8), :] = jnp.where(
            (ident == lane2 >> 2) & ((row2 & 3) == (lane2 & 3)), 1.0, 0.0)

    def source_wait(t, carry):
        source_copy(t, True).wait()
        return carry

    def ring_copy(slot, t, arriving):
        z = (my_z + t) % NZ
        at = z if arriving else my_z
        return pltpu.make_async_remote_copy(
            src_ref=mz.at[slot, at], dst_ref=mz.at[slot, at],
            send_sem=zs.at[slot, t], recv_sem=zq.at[slot, at],
            device_id=ring_peer(z), device_id_type=MESH)

    def ring_send(slot, value):
        mz[slot, my_z, 0:32] = value[:, :, 0:128].reshape(32, 128)
        packed = None
        for y in range(NY):
            part = jnp.where(lane == ID_LANE, ids[y], value[y, :, 128:256])
            part = pltpu.roll(part, 32 * y, 1) if y else part
            packed = part if packed is None else packed + part
        mz[slot, my_z, 32:40] = packed
        for t in (4, 3, 5, 2, 6, 1, 7):
            ring_copy(slot, t, False).start()

    def ring_wait(slot):
        for t in range(1, NZ):
            ring_copy(slot, t, True).wait()
        for z in range(NZ):
            cm[32 * z: 32 * z + 32, 0:128] = mz[slot, z, 0:32]
            packed = mz[slot, z, 32:40]
            for y in range(NY):
                at = 32 * z + 8 * y
                cm[at: at + 8, 128:256] = pltpu.roll(packed, 128 - 32 * y, 1) if y else packed

    def collect():
        hi, lo = halves(cm[...])
        return jnp.where(col < L, dot(pick[...], hi) + dot(pick[...], lo), 0.0)

    lax.fori_loop(1, NM, source_wait, 0)
    ring_send(0, jnp.sum(sr[...].astype(F32).reshape(NY, NCH, 8, 256), axis=1))
    ring_wait(0)
    ident = cm[:, 128 + ID_LANE: 128 + ID_LANE + 1].astype(jnp.int32)
    match = jnp.where((ident == col >> 2) & ((row & 3) == (col & 3)), 1.0, 0.0).astype(BF16)
    pick[...] = dot_t(eye[...], match).astype(BF16)
    r[...] = collect()

    def across(a):
        a = a + pltpu.roll(a, 64, 1)
        return a + pltpu.roll(a, 32, 1)

    def spread_near(grid):
        hi, lo = halves(grid)
        choose = own[...].astype(BF16)
        near_hi = dot(choose, hi).astype(BF16)
        near_lo = dot(choose, lo).astype(BF16)
        field = dot(near_hi, sh[...]) + dot(near_lo, sh[...]) + dot(near_hi, sl[...])
        ts[...] = field.reshape(NY, 8, 256)

    def widen(y):
        for h in range(LH):
            base = ts[y, :, 0:128] if h < 32 else ts[y, :, 128:256]
            fx[y, :, lanes(h)] = jnp.take_along_axis(base, 4 * (h % 32) + (lane >> 5), axis=1)

    def predict_one(m, y):
        parts = [None] * 4
        for h in range(LH):
            prod = jr[m, :, lanes(h)].astype(F32) * fx[y, :, lanes(h)]
            parts[h % 4] = prod if parts[h % 4] is None else parts[h % 4] + prod
        return across((parts[0] + parts[1]) + (parts[2] + parts[3]))

    def terms(slot):
        def group(y, carry):
            acc = []
            for h in range(LH):
                total = None
                for c in range(NCH):
                    prod = jr[y * NCH + c, :, lanes(h)].astype(F32) * sv[y * NCH + c]
                    total = prod if total is None else total + prod
                acc.append(total)
            hi, lo = halves(jnp.concatenate(acc, axis=0))
            sums = dot(hi, spot[...]) + dot(lo, spot[...])
            first = jnp.zeros((8, 128), F32)
            second = jnp.zeros((8, 128), F32)
            for h in range(LH):
                piece = jnp.where(lane >> 2 == h % 32, sums[8 * h: 8 * h + 8], 0.0)
                if h < 32:
                    first = first + piece
                else:
                    second = second + piece
            ts[y, :, 0:128] = first
            ts[y, :, 128:256] = second
            return carry

        lax.fori_loop(0, NY, group, 0)
        hi, lo = halves(ts[...].reshape(32, 256))
        back = dot_t(hi, sh[...]) + dot_t(lo, sh[...]) + dot_t(hi, sl[...])
        ring_send(slot, back.reshape(NY, 8, 256))

    spread_near(r[...])

    def widen_group(y, carry):
        widen(y)
        return carry

    lax.fori_loop(0, NY, widen_group, 0)

    def first_predict(m):
        extra = jr[m, :, lanes(LH - 1)].astype(F32)
        weights = across(jnp.where((lane >= 32) & (lane < 96), extra, 0.0))
        mw[m] = weights
        sv[m] = weights * predict_one(m, m // NCH)

    first_predict(my_m)

    def arrive(t, carry):
        m = (my_m + NM - t) % NM
        pltpu.make_async_remote_copy(
            src_ref=sb.at[m], dst_ref=jr.at[m], send_sem=js.at[m], recv_sem=jq.at[m],
            device_id=plane_peer(m), device_id_type=MESH).wait()
        first_predict(m)
        return carry

    lax.fori_loop(1, NM, arrive, 0)
    terms(1)
    p[...] = jnp.zeros_like(p)
    s[...] = jnp.zeros_like(s)
    x[...] = jnp.zeros_like(x)
    v[...] = jnp.zeros_like(v)
    ring_wait(1)
    w[...] = r[...] + collect()

    def plane_copy(slot, t, arriving):
        m = (my_m + t) % NM
        at = m if arriving else my_m
        return pltpu.make_async_remote_copy(
            src_ref=sx.at[slot, at], dst_ref=sx.at[slot, at],
            send_sem=xs.at[slot, m], recv_sem=xq.at[slot, at],
            device_id=plane_peer(m), device_id_type=MESH)

    def scalars_send(slot):
        res = r[...]
        norm = jnp.sum(res * res, axis=0, keepdims=True)
        norm = norm[:, 0:128] + norm[:, 128:256]
        bend = jnp.sum(res * w[...], axis=0, keepdims=True)
        bend = bend[:, 0:128] + bend[:, 128:256]
        sx[slot, my_m] = jnp.where(
            lane1 < 64, norm + pltpu.roll(norm, 64, 1), bend + pltpu.roll(bend, 64, 1))

        def start(t, carry):
            plane_copy(slot, t, False).start()
            return carry

        lax.fori_loop(1, NM, start, 0)

    def advance(i, slot, norm_old, step_old):
        def finish(t, carry):
            plane_copy(slot, t, True).wait()
            return carry

        lax.fori_loop(1, NM, finish, 0)
        both = jnp.sum(sx[slot], axis=0)
        norm = jnp.sum(jnp.where(lane1 < 64, both, 0.0), axis=1, keepdims=True)
        bend = jnp.sum(jnp.where(lane1 < 64, 0.0, both), axis=1, keepdims=True)
        ratio = jnp.where(i == 0, 0.0, norm / norm_old)
        step = norm / (bend - jnp.where(i == 0, 0.0, ratio * norm / step_old))
        turned = w[...] + ratio * s[...]
        s[...] = turned
        ahead = r[...] + ratio * p[...]
        p[...] = ahead
        x[...] = x[...] + step * ahead
        r[...] = r[...] - step * turned
        return norm, step, ratio

    def iteration(i, carry):
        slot = i & 1
        spread_near(w[...])
        scalars_send(slot)

        def predict(y, carry):
            widen(y)
            for c in range(NCH):
                m = y * NCH + c
                sv[m] = mw[m] * predict_one(m, y)
            return carry

        lax.fori_loop(0, NY, predict, 0)
        terms(slot)
        norm, step, ratio = advance(i, slot, *carry)
        ring_wait(slot)
        along = w[...] + collect() + ratio * v[...]
        v[...] = along
        w[...] = w[...] - step * along
        return norm, step

    one = jnp.ones((1, 1), F32)
    norm, step = lax.fori_loop(0, ITERS - 1, iteration, (one, one))
    scalars_send((ITERS - 1) & 1)
    advance(ITERS - 1, (ITERS - 1) & 1, norm, step)

    hi, lo = halves(x[...])
    grown = dot(hi, sh[...]) + dot(lo, sh[...]) + dot(hi, sl[...])
    out[:, 0:8, :] = grown.astype(BF16).reshape(NM, 8, 256)
    out[:, 8:16, :] = r[...].astype(BF16).reshape(NM, 8, 256)

    def result_copy(t, arriving):
        m = (my_m + t) % NM
        at = m if arriving else my_m
        return pltpu.make_async_remote_copy(
            src_ref=out.at[m // NCH * NZ + my_z], dst_ref=got.at[at],
            send_sem=os.at[m], recv_sem=oq.at[at],
            device_id=plane_peer(m), device_id_type=MESH)

    def give(t, carry):
        result_copy(t, False).start()
        return carry

    def take(t, carry):
        result_copy(t, True).wait()
        return carry

    lax.fori_loop(1, NM, give, 0)
    got[my_m] = out[my_y * NZ + my_z]
    lax.fori_loop(1, NM, take, 0)
    for k, ref in ((0, inc_ref), (1, res_ref)):
        rows = got[:, 8 * k: 8 * k + 8, :].reshape(256, 256)
        flat = dot_t(eye[0:144, :], rows).astype(BF16)
        ref[...] = dot(flat, perm[...])[0:L]


def per_device(jacobian, departures, obs_weights, column_count, grid_block, sqrt_cov):
    jt = jnp.transpose(jacobian, (2, 1, 0))
    vmem = pl.BlockSpec(memory_space=pltpu.VMEM)
    dma = pltpu.SemaphoreType.DMA
    state = pltpu.VMEM((256, 256), F32)
    table = pltpu.VMEM((256, 256), BF16)
    inc, res = pl.pallas_call(
        kernel,
        out_shape=(jax.ShapeDtypeStruct((L, 256), F32),) * 2,
        in_specs=[pl.BlockSpec(memory_space=pltpu.HBM)] * 6,
        out_specs=(vmem, vmem),
        scratch_shapes=[
            pltpu.SMEM((1,), jnp.int32),
            pltpu.SMEM((2,), jnp.int32),
            pltpu.VMEM((144, 32, 256), BF16),
            pltpu.VMEM((32, 256), F32),
            pltpu.VMEM((32, 256), F32),
            pltpu.VMEM((L, L), F32),
            pltpu.VMEM((NM, 8, WIDE), BF16),
            pltpu.VMEM((NM, 8, WIDE), BF16),
            pltpu.VMEM((NM, 8, 128), F32),
            pltpu.VMEM((NY, 8, WIDE), F32),
            pltpu.VMEM((NM, 8, 128), F32),
            pltpu.VMEM((NY, 8, 256), F32),
            table, table, table, table,
            pltpu.VMEM((128, 128), BF16),
            pltpu.VMEM((32, 256), F32),
            table,
            pltpu.VMEM((NY, 8, 128), F32),
            pltpu.VMEM((144, 256), F32),
            pltpu.VMEM((NM, 8, 256), BF16),
            pltpu.VMEM((NM, 8, 256), BF16),
            state,
            state, state, state, state, state, state,
            pltpu.VMEM((2, NZ, 40, 128), F32),
            pltpu.VMEM((2, NM, 1, 128), F32),
            pltpu.VMEM((NM, 16, 256), BF16),
            pltpu.VMEM((NM, 16, 256), BF16),
            dma((5 + CHUNKS,)),
            dma((NM,)), dma((NM,)),
            dma((NM,)), dma((NM,)),
            dma((2, NZ)), dma((2, NZ)),
            dma((2, NM)), dma((2, NM)),
            dma((NY,)), dma((NY,)),
            dma((NM,)), dma((NM,)),
        ],
        compiler_params=pltpu.CompilerParams(
            collective_id=0, has_side_effects=True, vmem_limit_bytes=67_000_000),
        name="cg",
    )(column_count, grid_block, jt, obs_weights, departures, sqrt_cov)
    return inc.T, res.T


def solution(mesh):
    split = Mesh(mesh.devices.reshape(NY, NZ, NX, NC), ("obs_0", "obs_1", "chan_0", "chan_1"))
    return jax.shard_map(
        per_device,
        mesh=split,
        in_specs=(P(OBS, CHAN, None), P(CHAN, OBS), P(CHAN, OBS), P(OBS), P(OBS), P()),
        out_specs=(P(OBS, None), P(OBS, None)),
        check_vma=False,
    )
```

```python
import jax
import jax.numpy as jnp
from jax import lax
from jax.experimental import pallas as pl
from jax.experimental.pallas import tpu as pltpu
from jax.sharding import Mesh
from jax.sharding import PartitionSpec as P

ITERS = 5
L = 137
NY, NZ, NX, NC = 4, 8, 4, 2
NCH = NX * NC
NM = NY * NCH
LH = 35
CHUNKS = 5
PER = LH // CHUNKS
WIDE = LH * 128
ID_LANE = 16
OBS = ("obs_0", "obs_1")
CHAN = ("chan_0", "chan_1")
MESH = pl.DeviceIdType.MESH
F32 = jnp.float32
BF16 = jnp.bfloat16


def iota(shape, dim):
    return lax.broadcasted_iota(jnp.int32, shape, dim)


def dot(a, b):
    return jnp.dot(a, b, preferred_element_type=F32)


def dot_t(a, b):
    return lax.dot_general(a, b, (((1,), (1,)), ((), ())), preferred_element_type=F32)


def halves(v):
    hi = v.astype(BF16)
    return hi, (v - hi.astype(F32)).astype(BF16)


def lanes(q):
    return pl.ds(q * 128, 128)


def kernel(
    cnt_hbm, gb_hbm, jt_hbm, w_hbm, d_hbm, s_hbm,
    inc_ref, res_ref,
    cnt_ref, gb_ref, jv, w_ref, d_ref, s_ref,
    sb, jr, jf, mw, fx, sv, ff, fv, sh, sl, qh, ql, perm, eye, spot, own, near, pick, ids, tt, so, sr, cm,
    r, p, s, x, w, v, g, mz, sx, out, got,
    fs, js, jq, as_, aq, zs, zq, xs, xq, ys, yq, os, oq,
):
    my_y = lax.axis_index("obs_0")
    my_z = lax.axis_index("obs_1")
    my_x = lax.axis_index("chan_0")
    my_c = lax.axis_index("chan_1")
    my_m = my_y * NCH + my_x * NC + my_c

    fetches = [
        pltpu.make_async_copy(a, b, fs.at[k])
        for k, (a, b) in enumerate((
            (w_hbm, w_ref), (d_hbm, d_ref), (cnt_hbm, cnt_ref), (gb_hbm, gb_ref), (s_hbm, s_ref)))
    ]
    blocks = []
    for q in range(CHUNKS):
        first, last = 4 * PER * q, min(4 * PER * (q + 1), L)
        blocks.append(pltpu.make_async_copy(
            jt_hbm.at[first:last], jv.at[first:last], fs.at[len(fetches) + q]))
    for copy in (blocks[0], *fetches, *blocks[1:]):
        copy.start()

    def plane_peer(m):
        return (m // NCH, my_z, (m % NCH) // NC, m % NC)

    def ring_peer(z):
        return (my_y, z, my_x, my_c)

    barrier = pltpu.get_barrier_semaphore()

    def greet_plane(t, carry):
        pl.semaphore_signal(barrier, inc=1, device_id=plane_peer((my_m + t) % NM), device_id_type=MESH)
        return carry

    def greet_ring(t, carry):
        pl.semaphore_signal(barrier, inc=1, device_id=ring_peer((my_z + t) % NZ), device_id_type=MESH)
        return carry

    lax.fori_loop(1, NM, greet_plane, 0)
    lax.fori_loop(1, NZ, greet_ring, 0)

    row = iota((256, 256), 0)
    col = iota((256, 256), 1)
    lane = iota((8, 128), 1)
    lane1 = iota((1, 128), 1)
    perm[...] = jnp.where(
        ((row & 4) << 5) + ((row >> 3) << 2) + (row & 3) == col, 1.0, 0.0).astype(BF16)
    jv[L:144] = jnp.zeros((144 - L, 32, 256), BF16)

    def turn(h, carry):
        block = jv[pl.ds(4 * h, 4)].reshape(128, 256)
        turned = dot_t(perm[...], block).astype(BF16)
        sb[:, :, pl.ds(pl.multiple_of(h * 128, 128), 128)] = turned.reshape(NM, 8, 128)
        return carry

    def send_part(first, last):
        part = pl.ds(first * 128, (last - first) * 128)

        def send(t, carry):
            m = (my_m + t) % NM
            pltpu.make_async_remote_copy(
                src_ref=sb.at[m, :, part], dst_ref=jr.at[my_m, :, part],
                send_sem=js.at[m], recv_sem=jq.at[my_m],
                device_id=plane_peer(m), device_id_type=MESH).start()
            return carry

        lax.fori_loop(1, NM, send, 0)

    blocks[0].wait()
    lax.fori_loop(0, PER, turn, 0, unroll=True)
    pl.semaphore_wait(barrier, NM - 1 + NZ - 1)
    send_part(0, PER)

    for copy in fetches:
        copy.wait()
    sh[...] = jnp.zeros_like(sh)
    sl[...] = jnp.zeros_like(sl)
    root_hi, root_lo = halves(s_ref[...])
    sh[0:L, 0:L] = root_hi
    sl[0:L, 0:L] = root_lo
    r4 = iota((8, 128), 0)
    ids[my_y] = jnp.where(r4 < 4, gb_ref[0], gb_ref[1]).astype(F32)

    def id_copy(t, arriving):
        peer = (my_y + t) % NY
        at = peer if arriving else my_y
        return pltpu.make_async_remote_copy(
            src_ref=ids.at[at], dst_ref=ids.at[at], send_sem=ys.at[t], recv_sem=yq.at[at],
            device_id=(peer, my_z, my_x, my_c), device_id_type=MESH)

    for t in range(1, NY):
        id_copy(t, False).start()

    mask = jnp.where(iota((32, 256), 1) < cnt_ref[0], 1.0, 0.0)
    weight = mask * w_ref[...]
    weight_hi, weight_lo = halves(weight)
    scaled_d = (weight * d_ref[...]).astype(BF16)
    d_ref[...] = scaled_d.astype(F32)

    for copy in blocks[1:]:
        copy.wait()

    def gather_source(g, carry):
        part = jv[pl.ds(8 * g, 8)].astype(F32) * d_ref[...][None]
        tt[pl.ds(pl.multiple_of(8 * g, 8), 8), :] = jnp.sum(part, axis=1)
        return carry

    lax.fori_loop(0, 18, gather_source, 0, unroll=2)
    hi, lo = halves(tt[...])
    flat = dot_t(perm[...], hi) + dot_t(perm[...], lo)
    so[...] = jnp.pad(flat, ((0, 0), (0, 112))).astype(BF16).reshape(NM, 8, 256)

    def source_copy(t, arriving):
        m = (my_m + t) % NM
        return pltpu.make_async_remote_copy(
            src_ref=so.at[m], dst_ref=sr.at[m if arriving else my_m],
            send_sem=as_.at[m], recv_sem=aq.at[m if arriving else my_m],
            device_id=plane_peer(m), device_id_type=MESH)

    def source_send(t, carry):
        source_copy(t, False).start()
        return carry

    lax.fori_loop(1, NM, source_send, 0)
    sr[my_m] = so[my_m]

    lax.fori_loop(PER, LH - 1, turn, 0, unroll=9)
    block = jnp.concatenate([jv[L - 1], weight_hi, weight_lo, jnp.zeros_like(weight_hi)], axis=0)
    sb[:, :, lanes(LH - 1)] = dot_t(perm[...], block).astype(BF16).reshape(NM, 8, 128)
    send_part(PER, LH)
    jr[my_m] = sb[my_m]

    eye[...] = jnp.where(row == col, 1.0, 0.0).astype(BF16)
    spot[...] = jnp.where(
        iota((128, 128), 0) >> 5 == (iota((128, 128), 1) & 3), 1.0, 0.0).astype(BF16)
    turned_hi = dot_t(eye[...], sh[...]).astype(BF16)
    turned_lo = dot_t(eye[...], sl[...]).astype(BF16)
    square = dot(turned_hi, sh[...]) + dot(turned_lo, sh[...]) + dot(turned_hi, sl[...])
    qh[...], ql[...] = halves(square)
    for t in range(1, NY):
        id_copy(t, True).wait()
    row2 = iota((8, 256), 0)
    lane2 = iota((8, 256), 1)
    for y in range(NY):
        ident = ids[y][:, 0:1].astype(jnp.int32)
        own[pl.ds(8 * y, 8), :] = jnp.where(
            (ident == lane2 >> 2) & ((row2 & 3) == (lane2 & 3)), 1.0, 0.0)

    def source_wait(t, carry):
        source_copy(t, True).wait()
        return carry

    def ring_copy(slot, t, arriving):
        z = (my_z + t) % NZ
        at = z if arriving else my_z
        return pltpu.make_async_remote_copy(
            src_ref=mz.at[slot, at], dst_ref=mz.at[slot, at],
            send_sem=zs.at[slot, t], recv_sem=zq.at[slot, at],
            device_id=ring_peer(z), device_id_type=MESH)

    def ring_start(slot, part):
        for t in (4, 3, 5, 2, 6, 1, 7):
            pltpu.make_async_remote_copy(
                src_ref=mz.at[slot, my_z, part], dst_ref=mz.at[slot, my_z, part],
                send_sem=zs.at[slot, t], recv_sem=zq.at[slot, my_z],
                device_id=ring_peer((my_z + t) % NZ), device_id_type=MESH).start()

    def ring_tail(slot, tails):
        packed = None
        for y in range(NY):
            part = jnp.where(lane == ID_LANE, ids[y], tails[y])
            part = pltpu.roll(part, 32 * y, 1) if y else part
            packed = part if packed is None else packed + part
        mz[slot, my_z, 32:40] = packed
        ring_start(slot, pl.ds(32, 8))

    def ring_wait(slot):
        for t in range(1, NZ):
            ring_copy(slot, t, True).wait()
        for z in range(NZ):
            cm[32 * z: 32 * z + 32, 0:128] = mz[slot, z, 0:32]
            packed = mz[slot, z, 32:40]
            for y in range(NY):
                at = 32 * z + 8 * y
                cm[at: at + 8, 128:256] = pltpu.roll(packed, 128 - 32 * y, 1) if y else packed

    def times(a, hi_ref, lo_ref):
        hi, lo = halves(a)
        return dot(hi, hi_ref[...]) + dot(lo, hi_ref[...]) + dot(hi, lo_ref[...])

    def collect():
        hi, lo = halves(cm[...])
        close = times(dot(near[...], hi) + dot(near[...], lo), qh, ql)
        hi, lo = halves(dot(pick[...], hi) + dot(pick[...], lo))
        return dot_t(hi, sh[...]) + dot_t(lo, sh[...]) + dot_t(hi, sl[...]), close.reshape(NY, 8, 256)

    lax.fori_loop(1, NM, source_wait, 0)
    arrived = jnp.sum(sr[...].astype(F32).reshape(NY, NCH, 8, 256), axis=1)
    mz[0, my_z, 0:32] = arrived[:, :, 0:128].reshape(32, 128)
    ring_start(0, pl.ds(0, 32))
    ring_tail(0, arrived[:, :, 128:256])
    ring_wait(0)
    ident = cm[:, 128 + ID_LANE: 128 + ID_LANE + 1].astype(jnp.int32)
    match = jnp.where((ident == col >> 2) & ((row & 3) == (col & 3)), 1.0, 0.0).astype(BF16)
    pick[...] = dot_t(eye[...], match).astype(BF16)
    near[...] = dot_t(own[...].astype(BF16), match).astype(BF16)
    start_r, start_f = collect()
    r[...] = start_r
    ff[...] = start_f

    def across(a):
        a = a + pltpu.roll(a, 64, 1)
        return a + pltpu.roll(a, 32, 1)

    def widen(y):
        for h in range(LH):
            base = ff[y, :, 0:128] if h < 32 else ff[y, :, 128:256]
            fx[y, :, lanes(h)] = jnp.take_along_axis(base, 4 * (h % 32) + (lane >> 5), axis=1)

    def group_terms(slot, y, factors):
        acc = []
        for h in range(LH):
            total = None
            for c in range(NCH):
                prod = jf[y * NCH + c, :, lanes(h)] * factors[c]
                total = prod if total is None else total + prod
            acc.append(total)
        hi, lo = halves(jnp.concatenate(acc, axis=0))
        sums = dot(hi, spot[...]) + dot(lo, spot[...])
        first = jnp.zeros((8, 128), F32)
        second = jnp.zeros((8, 128), F32)
        for h in range(LH):
            piece = jnp.where(lane >> 2 == h % 32, sums[8 * h: 8 * h + 8], 0.0)
            if h < 32:
                first = first + piece
            else:
                second = second + piece
        part = pl.ds(pl.multiple_of(8 * y, 8), 8)
        mz[slot, my_z, part] = first
        g[part, 0:128] = second
        ring_start(slot, part)

    def send_tail(slot):
        ring_tail(slot, [g[8 * y: 8 * y + 8, 0:128] for y in range(NY)])

    def widen_group(y, carry):
        widen(y)
        return carry

    lax.fori_loop(0, NY, widen_group, 0)

    def first_predict(m):
        y = m // NCH
        extra = jr[m, :, lanes(LH - 1)].astype(F32)
        weights = across(jnp.where((lane >= 32) & (lane < 96), extra, 0.0))
        mw[m] = weights
        parts = [None] * 4
        for h in range(LH):
            tile = jr[m, :, lanes(h)].astype(F32)
            if h == LH - 1:
                tile = jnp.where(lane < 32, tile, 0.0)
            jf[m, :, lanes(h)] = tile
            prod = tile * fx[y, :, lanes(h)]
            parts[h % 4] = prod if parts[h % 4] is None else parts[h % 4] + prod
        sv[m] = weights * across((parts[0] + parts[1]) + (parts[2] + parts[3]))

    first_predict(my_m)

    def arrive(t, carry):
        m = (my_m + NM - t) % NM
        pltpu.make_async_remote_copy(
            src_ref=sb.at[m], dst_ref=jr.at[m], send_sem=js.at[m], recv_sem=jq.at[m],
            device_id=plane_peer(m), device_id_type=MESH).wait()
        first_predict(m)
        return carry

    lax.fori_loop(1, NM, arrive, 0)

    def first_group(y, carry):
        group_terms(1, y, [sv[y * NCH + c] for c in range(NCH)])
        return carry

    lax.fori_loop(0, NY, first_group, 0)
    send_tail(1)
    p[...] = jnp.zeros_like(p)
    s[...] = jnp.zeros_like(s)
    x[...] = jnp.zeros_like(x)
    v[...] = jnp.zeros_like(v)
    fv[...] = jnp.zeros_like(fv)
    ring_wait(1)
    more, close = collect()
    ff[...] = ff[...] + close
    w[...] = r[...] + more

    def plane_copy(slot, t, arriving):
        m = (my_m + t) % NM
        at = m if arriving else my_m
        return pltpu.make_async_remote_copy(
            src_ref=sx.at[slot, at], dst_ref=sx.at[slot, at],
            send_sem=xs.at[slot, m], recv_sem=xq.at[slot, at],
            device_id=plane_peer(m), device_id_type=MESH)

    def scalars_send(slot):
        res = r[...]
        norm = jnp.sum(res * res, axis=0, keepdims=True)
        norm = norm[:, 0:128] + norm[:, 128:256]
        bend = jnp.sum(res * w[...], axis=0, keepdims=True)
        bend = bend[:, 0:128] + bend[:, 128:256]
        sx[slot, my_m] = jnp.where(
            lane1 < 64, norm + pltpu.roll(norm, 64, 1), bend + pltpu.roll(bend, 64, 1))

        def start(t, carry):
            plane_copy(slot, t, False).start()
            return carry

        lax.fori_loop(1, NM, start, 0)

    def scalars_wait(i, slot, norm_old, step_old):
        def finish(t, carry):
            plane_copy(slot, t, True).wait()
            return carry

        lax.fori_loop(1, NM, finish, 0)
        both = jnp.sum(sx[slot], axis=0)
        norm = jnp.sum(jnp.where(lane1 < 64, both, 0.0), axis=1, keepdims=True)
        bend = jnp.sum(jnp.where(lane1 < 64, 0.0, both), axis=1, keepdims=True)
        ratio = jnp.where(i == 0, 0.0, norm / norm_old)
        step = norm / (bend - jnp.where(i == 0, 0.0, ratio * norm / step_old))
        return norm, step, ratio

    def iteration(i, carry):
        slot = i & 1
        scalars_send(slot)

        def group(y, carry):
            widen(y)
            totals = [None] * NCH
            for h in range(LH):
                wide = fx[y, :, lanes(h)]
                for c in range(NCH):
                    prod = jf[y * NCH + c, :, lanes(h)] * wide
                    totals[c] = prod if totals[c] is None else totals[c] + prod
            group_terms(slot, y, [mw[y * NCH + c] * across(totals[c]) for c in range(NCH)])
            return carry

        lax.fori_loop(0, NY, group, 0)
        send_tail(slot)
        norm, step, ratio = scalars_wait(i, slot, *carry)
        turned = w[...] + ratio * s[...]
        s[...] = turned
        ahead = r[...] + ratio * p[...]
        p[...] = ahead
        x[...] = x[...] + step * ahead
        r[...] = r[...] - step * turned
        ring_wait(slot)
        more, close = collect()
        along = ff[...] + close + ratio * fv[...]
        fv[...] = along
        ff[...] = ff[...] - step * along
        along = w[...] + more + ratio * v[...]
        v[...] = along
        w[...] = w[...] - step * along
        return norm, step

    one = jnp.ones((1, 1), F32)
    norm, step = lax.fori_loop(0, ITERS - 1, iteration, (one, one))
    last = ITERS - 1
    scalars_send(last & 1)
    cm[...] = times(r[...], sh, sl)
    v[...] = times(p[...], sh, sl)
    g[...] = times(x[...], sh, sl)
    norm, step, ratio = scalars_wait(last, last & 1, norm, step)
    grown = g[...] + step * (cm[...] + ratio * v[...])
    left = r[...] - step * (w[...] + ratio * s[...])
    out[:, 0:8, :] = grown.astype(BF16).reshape(NM, 8, 256)
    out[:, 8:16, :] = left.astype(BF16).reshape(NM, 8, 256)

    def result_copy(t, arriving):
        m = (my_m + t) % NM
        at = m if arriving else my_m
        return pltpu.make_async_remote_copy(
            src_ref=out.at[m // NCH * NZ + my_z], dst_ref=got.at[at],
            send_sem=os.at[m], recv_sem=oq.at[at],
            device_id=plane_peer(m), device_id_type=MESH)

    def give(t, carry):
        result_copy(t, False).start()
        return carry

    def take(t, carry):
        result_copy(t, True).wait()
        return carry

    lax.fori_loop(1, NM, give, 0)
    got[my_m] = out[my_y * NZ + my_z]
    lax.fori_loop(1, NM, take, 0)
    for k, ref in ((0, inc_ref), (1, res_ref)):
        rows = got[:, 8 * k: 8 * k + 8, :].reshape(256, 256)
        flat = dot_t(eye[0:144, :], rows).astype(BF16)
        ref[...] = dot(flat, perm[...])[0:L]


def per_device(jacobian, departures, obs_weights, column_count, grid_block, sqrt_cov):
    jt = jnp.transpose(jacobian, (2, 1, 0))
    vmem = pl.BlockSpec(memory_space=pltpu.VMEM)
    dma = pltpu.SemaphoreType.DMA
    state = pltpu.VMEM((256, 256), F32)
    table = pltpu.VMEM((256, 256), BF16)
    inc, res = pl.pallas_call(
        kernel,
        out_shape=(jax.ShapeDtypeStruct((L, 256), F32),) * 2,
        in_specs=[pl.BlockSpec(memory_space=pltpu.HBM)] * 6,
        out_specs=(vmem, vmem),
        scratch_shapes=[
            pltpu.SMEM((1,), jnp.int32),
            pltpu.SMEM((2,), jnp.int32),
            pltpu.VMEM((144, 32, 256), BF16),
            pltpu.VMEM((32, 256), F32),
            pltpu.VMEM((32, 256), F32),
            pltpu.VMEM((L, L), F32),
            pltpu.VMEM((NM, 8, WIDE), BF16),
            pltpu.VMEM((NM, 8, WIDE), BF16),
            pltpu.VMEM((NM, 8, WIDE), F32),
            pltpu.VMEM((NM, 8, 128), F32),
            pltpu.VMEM((NY, 8, WIDE), F32),
            pltpu.VMEM((NM, 8, 128), F32),
            pltpu.VMEM((NY, 8, 256), F32),
            pltpu.VMEM((NY, 8, 256), F32),
            table, table, table, table, table, table,
            pltpu.VMEM((128, 128), BF16),
            pltpu.VMEM((32, 256), F32),
            pltpu.VMEM((32, 256), BF16),
            table,
            pltpu.VMEM((NY, 8, 128), F32),
            pltpu.VMEM((144, 256), F32),
            pltpu.VMEM((NM, 8, 256), BF16),
            pltpu.VMEM((NM, 8, 256), BF16),
            state,
            state, state, state, state, state, state, state,
            pltpu.VMEM((2, NZ, 40, 128), F32),
            pltpu.VMEM((2, NM, 1, 128), F32),
            pltpu.VMEM((NM, 16, 256), BF16),
            pltpu.VMEM((NM, 16, 256), BF16),
            dma((5 + CHUNKS,)),
            dma((NM,)), dma((NM,)),
            dma((NM,)), dma((NM,)),
            dma((2, NZ)), dma((2, NZ)),
            dma((2, NM)), dma((2, NM)),
            dma((NY,)), dma((NY,)),
            dma((NM,)), dma((NM,)),
        ],
        compiler_params=pltpu.CompilerParams(
            collective_id=0, has_side_effects=True, vmem_limit_bytes=67_000_000),
        name="cg",
    )(column_count, grid_block, jt, obs_weights, departures, sqrt_cov)
    return inc.T, res.T


def solution(mesh):
    split = Mesh(mesh.devices.reshape(NY, NZ, NX, NC), ("obs_0", "obs_1", "chan_0", "chan_1"))
    return jax.shard_map(
        per_device,
        mesh=split,
        in_specs=(P(OBS, CHAN, None), P(CHAN, OBS), P(CHAN, OBS), P(OBS), P(OBS), P()),
        out_specs=(P(OBS, None), P(OBS, None)),
        check_vma=False,
    )
```

```python
import functools

import jax
import jax.numpy as jnp
from jax import lax
from jax.experimental import pallas as pl
from jax.experimental.pallas import tpu as pltpu
from jax.sharding import Mesh
from jax.sharding import PartitionSpec as P

ITERS = 5
L = 137
NY, NZ, NX, NC = 4, 8, 4, 2
NCH = NX * NC
NM = NY * NCH
LH = 35
CHUNKS = 5
PER = LH // CHUNKS
WIDE = LH * 128
ID_LANE = 16
OBS = ("obs_0", "obs_1")
CHAN = ("chan_0", "chan_1")
MESH = pl.DeviceIdType.MESH
F32 = jnp.float32
BF16 = jnp.bfloat16


def iota(shape, dim):
    return lax.broadcasted_iota(jnp.int32, shape, dim)


def dot(a, b):
    return jnp.dot(a, b, preferred_element_type=F32)


def dot_t(a, b):
    return lax.dot_general(a, b, (((1,), (1,)), ((), ())), preferred_element_type=F32)


def halves(v):
    hi = v.astype(BF16)
    return hi, (v - hi.astype(F32)).astype(BF16)


def lanes(q):
    return pl.ds(q * 128, 128)


def kernel(
    cnt_hbm, gb_hbm, jt_hbm, w_hbm, d_hbm, s_hbm,
    got_ref,
    cnt_ref, gb_ref, jv, w_ref, d_ref, s_ref,
    sb, jr, jf, mw, fx, sv, ff, fv, sh, sl, qh, ql, perm, eye, spot, own, near, pick, ids, tt, so, sr, cm,
    r, p, s, x, w, v, g, mz, sx, out, got,
    fs, js, jq, as_, aq, zs, zq, xs, xq, ys, yq, os, oq,
):
    my_y = lax.axis_index("obs_0")
    my_z = lax.axis_index("obs_1")
    my_x = lax.axis_index("chan_0")
    my_c = lax.axis_index("chan_1")
    my_m = my_y * NCH + my_x * NC + my_c

    fetches = [
        pltpu.make_async_copy(a, b, fs.at[k])
        for k, (a, b) in enumerate((
            (w_hbm, w_ref), (d_hbm, d_ref), (cnt_hbm, cnt_ref), (gb_hbm, gb_ref), (s_hbm, s_ref)))
    ]
    blocks = [
        pltpu.make_async_copy(jt_hbm.at[first:last], jv.at[first:last], fs.at[len(fetches) + q])
        for q, (first, last) in enumerate(((0, 4 * PER), (4 * PER, L)))
    ]
    for copy in (blocks[0], *fetches, *blocks[1:]):
        copy.start()

    def plane_peer(m):
        return (m // NCH, my_z, (m % NCH) // NC, m % NC)

    def ring_peer(z):
        return (my_y, z, my_x, my_c)

    barrier = pltpu.get_barrier_semaphore()

    def greet_plane(t, carry):
        pl.semaphore_signal(barrier, inc=1, device_id=plane_peer((my_m + t) % NM), device_id_type=MESH)
        return carry

    def greet_ring(t, carry):
        pl.semaphore_signal(barrier, inc=1, device_id=ring_peer((my_z + t) % NZ), device_id_type=MESH)
        return carry

    lax.fori_loop(1, NM, greet_plane, 0)
    lax.fori_loop(1, NZ, greet_ring, 0)

    row = iota((256, 256), 0)
    col = iota((256, 256), 1)
    lane = iota((8, 128), 1)
    lane1 = iota((1, 128), 1)
    perm[...] = jnp.where(
        ((row & 4) << 5) + ((row >> 3) << 2) + (row & 3) == col, 1.0, 0.0).astype(BF16)
    jv[L:144] = jnp.zeros((144 - L, 32, 256), BF16)

    def turn(h, carry):
        block = jv[pl.ds(4 * h, 4)].reshape(128, 256)
        turned = dot_t(perm[...], block).astype(BF16)
        sb[:, :, pl.ds(pl.multiple_of(h * 128, 128), 128)] = turned.reshape(NM, 8, 128)
        return carry

    def chunk(q):
        return pl.ds(q * PER * 128, PER * 128)

    def send_chunk(q):
        def send(t, carry):
            m = (my_m + t) % NM
            pltpu.make_async_remote_copy(
                src_ref=sb.at[m, :, chunk(q)], dst_ref=jr.at[my_m, :, chunk(q)],
                send_sem=js.at[m], recv_sem=jq.at[q, my_m],
                device_id=plane_peer(m), device_id_type=MESH).start()
            return carry

        lax.fori_loop(1, NM, send, 0)

    def chunk_wait(q, m):
        pltpu.make_async_remote_copy(
            src_ref=sb.at[m, :, chunk(q)], dst_ref=jr.at[m, :, chunk(q)],
            send_sem=js.at[m], recv_sem=jq.at[q, m],
            device_id=plane_peer(m), device_id_type=MESH).wait_recv()

    blocks[0].wait()
    lax.fori_loop(0, PER, turn, 0, unroll=True)
    pl.semaphore_wait(barrier, NM - 1 + NZ - 1)
    send_chunk(0)

    for copy in fetches:
        copy.wait()
    sh[...] = jnp.zeros_like(sh)
    sl[...] = jnp.zeros_like(sl)
    root_hi, root_lo = halves(s_ref[...])
    sh[0:L, 0:L] = root_hi
    sl[0:L, 0:L] = root_lo
    r4 = iota((8, 128), 0)
    ids[my_y] = jnp.where(r4 < 4, gb_ref[0], gb_ref[1]).astype(F32)

    def id_copy(t, arriving):
        peer = (my_y + t) % NY
        at = peer if arriving else my_y
        return pltpu.make_async_remote_copy(
            src_ref=ids.at[at], dst_ref=ids.at[at], send_sem=ys.at[t], recv_sem=yq.at[at],
            device_id=(peer, my_z, my_x, my_c), device_id_type=MESH)

    for t in range(1, NY):
        id_copy(t, False).start()

    mask = jnp.where(iota((32, 256), 1) < cnt_ref[0], 1.0, 0.0)
    weight = mask * w_ref[...]
    weight_hi, weight_lo = halves(weight)
    scaled_d = (weight * d_ref[...]).astype(BF16)
    d_ref[...] = scaled_d.astype(F32)

    for copy in blocks[1:]:
        copy.wait()

    def gather_source(g, carry):
        part = jv[pl.ds(8 * g, 8)].astype(F32) * d_ref[...][None]
        tt[pl.ds(pl.multiple_of(8 * g, 8), 8), :] = jnp.sum(part, axis=1)
        return carry

    lax.fori_loop(0, 18, gather_source, 0, unroll=2)
    hi, lo = halves(tt[...])
    flat = dot_t(perm[...], hi) + dot_t(perm[...], lo)
    so[...] = jnp.pad(flat, ((0, 0), (0, 112))).astype(BF16).reshape(NM, 8, 256)

    def source_copy(t, arriving):
        m = (my_m + t) % NM
        return pltpu.make_async_remote_copy(
            src_ref=so.at[m], dst_ref=sr.at[m if arriving else my_m],
            send_sem=as_.at[m], recv_sem=aq.at[m if arriving else my_m],
            device_id=plane_peer(m), device_id_type=MESH)

    def source_send(t, carry):
        source_copy(t, False).start()
        return carry

    lax.fori_loop(1, NM, source_send, 0)
    sr[my_m] = so[my_m]

    for q in range(1, CHUNKS):
        if q < CHUNKS - 1:
            lax.fori_loop(q * PER, (q + 1) * PER, turn, 0, unroll=True)
        else:
            lax.fori_loop(q * PER, LH - 1, turn, 0, unroll=True)
            block = jnp.concatenate([jv[L - 1], weight_hi, weight_lo, jnp.zeros_like(weight_hi)], axis=0)
            sb[:, :, lanes(LH - 1)] = dot_t(perm[...], block).astype(BF16).reshape(NM, 8, 128)
        send_chunk(q)
    jr[my_m] = sb[my_m]

    eye[...] = jnp.where(row == col, 1.0, 0.0).astype(BF16)
    spot[...] = jnp.where(
        iota((128, 128), 0) >> 5 == (iota((128, 128), 1) & 3), 1.0, 0.0).astype(BF16)
    turned_hi = dot_t(eye[...], sh[...]).astype(BF16)
    turned_lo = dot_t(eye[...], sl[...]).astype(BF16)
    square = dot(turned_hi, sh[...]) + dot(turned_lo, sh[...]) + dot(turned_hi, sl[...])
    qh[...], ql[...] = halves(square)
    for t in range(1, NY):
        id_copy(t, True).wait()
    row2 = iota((8, 256), 0)
    lane2 = iota((8, 256), 1)
    for y in range(NY):
        ident = ids[y][:, 0:1].astype(jnp.int32)
        own[pl.ds(8 * y, 8), :] = jnp.where(
            (ident == lane2 >> 2) & ((row2 & 3) == (lane2 & 3)), 1.0, 0.0)

    def source_wait(t, carry):
        source_copy(t, True).wait()
        return carry

    def ring_copy(slot, t, arriving):
        z = (my_z + t) % NZ
        at = z if arriving else my_z
        return pltpu.make_async_remote_copy(
            src_ref=mz.at[slot, at], dst_ref=mz.at[slot, at],
            send_sem=zs.at[slot, t], recv_sem=zq.at[slot, at],
            device_id=ring_peer(z), device_id_type=MESH)

    def ring_start(slot, part):
        for t in (4, 3, 5, 2, 6, 1, 7):
            pltpu.make_async_remote_copy(
                src_ref=mz.at[slot, my_z, part], dst_ref=mz.at[slot, my_z, part],
                send_sem=zs.at[slot, t], recv_sem=zq.at[slot, my_z],
                device_id=ring_peer((my_z + t) % NZ), device_id_type=MESH).start()

    def ring_tail(slot, tails):
        packed = None
        for y in range(NY):
            part = jnp.where(lane == ID_LANE, ids[y], tails[y])
            part = pltpu.roll(part, 32 * y, 1) if y else part
            packed = part if packed is None else packed + part
        mz[slot, my_z, 32:40] = packed
        ring_start(slot, pl.ds(32, 8))

    def ring_wait(slot):
        for t in range(1, NZ):
            ring_copy(slot, t, True).wait()
        for z in range(NZ):
            cm[32 * z: 32 * z + 32, 0:128] = mz[slot, z, 0:32]
            packed = mz[slot, z, 32:40]
            for y in range(NY):
                at = 32 * z + 8 * y
                cm[at: at + 8, 128:256] = pltpu.roll(packed, 128 - 32 * y, 1) if y else packed

    def times(a, hi_ref, lo_ref):
        hi, lo = halves(a)
        return dot(hi, hi_ref[...]) + dot(lo, hi_ref[...]) + dot(hi, lo_ref[...])

    def collect():
        hi, lo = halves(cm[...])
        close = times(dot(near[...], hi) + dot(near[...], lo), qh, ql)
        hi, lo = halves(dot(pick[...], hi) + dot(pick[...], lo))
        return dot_t(hi, sh[...]) + dot_t(lo, sh[...]) + dot_t(hi, sl[...]), close.reshape(NY, 8, 256)

    def across(a):
        a = a + pltpu.roll(a, 64, 1)
        return a + pltpu.roll(a, 32, 1)

    def convert(q, m):
        tile = jr[m, :, chunk(q)].astype(F32)
        if q == CHUNKS - 1:
            extra = tile[:, (PER - 1) * 128:]
            mw[m] = across(jnp.where((lane >= 32) & (lane < 96), extra, 0.0))
            tile = jnp.concatenate([tile[:, : (PER - 1) * 128], jnp.where(lane < 32, extra, 0.0)], axis=1)
        jf[m, :, chunk(q)] = tile
        return tile

    def predict_part(q, m, tile):
        wide = tile * fx[m // NCH, :, chunk(q)]
        total = wide[:, 0:128]
        for h in range(1, PER):
            total = total + wide[:, 128 * h: 128 * h + 128]
        sv[m] = total if q == 0 else sv[m] + total

    def every_piece(q, work, waits):
        def pair(t, carry):
            m = (my_m + NM - 2 * t) % NM
            n = (my_m + NM - 2 * t - 1) % NM
            if waits:
                chunk_wait(q, m)
                chunk_wait(q, n)
            work(m)
            work(n)
            return carry

        first = (my_m + NM - 1) % NM
        if waits:
            chunk_wait(q, first)
        work(my_m)
        work(first)
        lax.fori_loop(1, NM // 2, pair, 0)

    every_piece(0, functools.partial(convert, 0), True)
    lax.fori_loop(1, NM, source_wait, 0)
    arrived = jnp.sum(sr[...].astype(F32).reshape(NY, NCH, 8, 256), axis=1)
    mz[0, my_z, 0:32] = arrived[:, :, 0:128].reshape(32, 128)
    ring_start(0, pl.ds(0, 32))
    ring_tail(0, arrived[:, :, 128:256])
    every_piece(1, functools.partial(convert, 1), True)
    ring_wait(0)
    ident = cm[:, 128 + ID_LANE: 128 + ID_LANE + 1].astype(jnp.int32)
    match = jnp.where((ident == col >> 2) & ((row & 3) == (col & 3)), 1.0, 0.0).astype(BF16)
    pick[...] = dot_t(eye[...], match).astype(BF16)
    near[...] = dot_t(own[...].astype(BF16), match).astype(BF16)
    start_r, start_f = collect()
    r[...] = start_r
    ff[...] = start_f

    def widen(y):
        for h in range(LH):
            base = ff[y, :, 0:128] if h < 32 else ff[y, :, 128:256]
            fx[y, :, lanes(h)] = jnp.take_along_axis(base, 4 * (h % 32) + (lane >> 5), axis=1)

    def group_terms(slot, y, factors):
        acc = []
        for h in range(LH):
            total = None
            for c in range(NCH):
                prod = jf[y * NCH + c, :, lanes(h)] * factors[c]
                total = prod if total is None else total + prod
            acc.append(total)
        hi, lo = halves(jnp.concatenate(acc, axis=0))
        sums = dot(hi, spot[...]) + dot(lo, spot[...])
        first = jnp.zeros((8, 128), F32)
        second = jnp.zeros((8, 128), F32)
        for h in range(LH):
            piece = jnp.where(lane >> 2 == h % 32, sums[8 * h: 8 * h + 8], 0.0)
            if h < 32:
                first = first + piece
            else:
                second = second + piece
        part = pl.ds(pl.multiple_of(8 * y, 8), 8)
        mz[slot, my_z, part] = first
        g[part, 0:128] = second
        ring_start(slot, part)

    def send_tail(slot):
        ring_tail(slot, [g[8 * y: 8 * y + 8, 0:128] for y in range(NY)])

    def widen_group(y, carry):
        widen(y)
        return carry

    lax.fori_loop(0, NY, widen_group, 0)

    for q in (0, 1):
        every_piece(q, lambda m: predict_part(q, m, jf[m, :, chunk(q)]), False)
    for q in range(2, CHUNKS):
        every_piece(q, lambda m: predict_part(q, m, convert(q, m)), True)

    def sent(t, carry):
        m = (my_m + t) % NM
        pltpu.make_async_remote_copy(
            src_ref=sb.at[m], dst_ref=jr.at[m], send_sem=js.at[m], recv_sem=jq.at[0, m],
            device_id=plane_peer(m), device_id_type=MESH).wait_send()
        return carry

    def first_group(y, carry):
        group_terms(1, y, [mw[y * NCH + c] * across(sv[y * NCH + c]) for c in range(NCH)])
        return carry

    lax.fori_loop(0, NY, first_group, 0)
    send_tail(1)
    lax.fori_loop(1, NM, sent, 0)
    p[...] = jnp.zeros_like(p)
    s[...] = jnp.zeros_like(s)
    x[...] = jnp.zeros_like(x)
    v[...] = jnp.zeros_like(v)
    fv[...] = jnp.zeros_like(fv)
    ring_wait(1)
    more, close = collect()
    ff[...] = ff[...] + close
    w[...] = r[...] + more

    def plane_copy(slot, t, arriving):
        m = (my_m + t) % NM
        at = m if arriving else my_m
        return pltpu.make_async_remote_copy(
            src_ref=sx.at[slot, at], dst_ref=sx.at[slot, at],
            send_sem=xs.at[slot, m], recv_sem=xq.at[slot, at],
            device_id=plane_peer(m), device_id_type=MESH)

    def scalars_send(slot):
        res = r[...]
        norm = jnp.sum(res * res, axis=0, keepdims=True)
        norm = norm[:, 0:128] + norm[:, 128:256]
        bend = jnp.sum(res * w[...], axis=0, keepdims=True)
        bend = bend[:, 0:128] + bend[:, 128:256]
        sx[slot, my_m] = jnp.where(
            lane1 < 64, norm + pltpu.roll(norm, 64, 1), bend + pltpu.roll(bend, 64, 1))

        def start(t, carry):
            plane_copy(slot, t, False).start()
            return carry

        lax.fori_loop(1, NM, start, 0)

    def scalars_wait(i, slot, norm_old, step_old):
        def finish(t, carry):
            plane_copy(slot, t, True).wait()
            return carry

        lax.fori_loop(1, NM, finish, 0)
        both = jnp.sum(sx[slot], axis=0)
        norm = jnp.sum(jnp.where(lane1 < 64, both, 0.0), axis=1, keepdims=True)
        bend = jnp.sum(jnp.where(lane1 < 64, 0.0, both), axis=1, keepdims=True)
        ratio = jnp.where(i == 0, 0.0, norm / norm_old)
        step = norm / (bend - jnp.where(i == 0, 0.0, ratio * norm / step_old))
        return norm, step, ratio

    def iteration(i, carry):
        slot = i & 1
        scalars_send(slot)

        def group(y, carry):
            widen(y)
            totals = [None] * NCH
            for h in range(LH):
                wide = fx[y, :, lanes(h)]
                for c in range(NCH):
                    prod = jf[y * NCH + c, :, lanes(h)] * wide
                    totals[c] = prod if totals[c] is None else totals[c] + prod
            group_terms(slot, y, [mw[y * NCH + c] * across(totals[c]) for c in range(NCH)])
            return carry

        lax.fori_loop(0, NY, group, 0)
        send_tail(slot)
        norm, step, ratio = scalars_wait(i, slot, *carry)
        turned = w[...] + ratio * s[...]
        s[...] = turned
        ahead = r[...] + ratio * p[...]
        p[...] = ahead
        x[...] = x[...] + step * ahead
        r[...] = r[...] - step * turned
        ring_wait(slot)
        more, close = collect()
        along = ff[...] + close + ratio * fv[...]
        fv[...] = along
        ff[...] = ff[...] - step * along
        along = w[...] + more + ratio * v[...]
        v[...] = along
        w[...] = w[...] - step * along
        return norm, step

    one = jnp.ones((1, 1), F32)
    norm, step = lax.fori_loop(0, ITERS - 1, iteration, (one, one))
    last = ITERS - 1
    scalars_send(last & 1)
    cm[...] = times(r[...], sh, sl)
    v[...] = times(p[...], sh, sl)
    g[...] = times(x[...], sh, sl)
    norm, step, ratio = scalars_wait(last, last & 1, norm, step)
    grown = g[...] + step * (cm[...] + ratio * v[...])
    left = r[...] - step * (w[...] + ratio * s[...])
    out[:, 0:8, :] = grown.astype(BF16).reshape(NM, 8, 256)
    out[:, 8:16, :] = left.astype(BF16).reshape(NM, 8, 256)

    def result_copy(t, arriving):
        m = (my_m + t) % NM
        at = m if arriving else my_m
        return pltpu.make_async_remote_copy(
            src_ref=out.at[m // NCH * NZ + my_z], dst_ref=got.at[at],
            send_sem=os.at[m], recv_sem=oq.at[at],
            device_id=plane_peer(m), device_id_type=MESH)

    def give(t, carry):
        result_copy(t, False).start()
        return carry

    def take(t, carry):
        result_copy(t, True).wait()
        return carry

    lax.fori_loop(1, NM, give, 0)
    got[my_m] = out[my_y * NZ + my_z]
    lax.fori_loop(1, NM, take, 0)
    got_ref[...] = got[...]


def finish(got_ref, inc_ref, res_ref):
    row = iota((256, 256), 0)
    col = iota((256, 256), 1)
    order = jnp.where(
        ((row & 4) << 5) + ((row >> 3) << 2) + (row & 3) == col, 1.0, 0.0).astype(BF16)
    eye = jnp.where(iota((144, 256), 0) == iota((144, 256), 1), 1.0, 0.0).astype(BF16)
    for k, ref in ((0, inc_ref), (1, res_ref)):
        rows = got_ref[:, 8 * k: 8 * k + 8, :].reshape(256, 256)
        ref[...] = dot(dot_t(eye, rows).astype(BF16), order)[0:L]


def per_device(jacobian, departures, obs_weights, column_count, grid_block, sqrt_cov):
    jt = jnp.transpose(jacobian, (2, 1, 0))
    vmem = pl.BlockSpec(memory_space=pltpu.VMEM)
    dma = pltpu.SemaphoreType.DMA
    state = pltpu.VMEM((256, 256), F32)
    table = pltpu.VMEM((256, 256), BF16)
    got = pl.pallas_call(
        kernel,
        out_shape=jax.ShapeDtypeStruct((NM, 16, 256), BF16),
        in_specs=[pl.BlockSpec(memory_space=pltpu.HBM)] * 6,
        out_specs=vmem,
        scratch_shapes=[
            pltpu.SMEM((1,), jnp.int32),
            pltpu.SMEM((2,), jnp.int32),
            pltpu.VMEM((144, 32, 256), BF16),
            pltpu.VMEM((32, 256), F32),
            pltpu.VMEM((32, 256), F32),
            pltpu.VMEM((L, L), F32),
            pltpu.VMEM((NM, 8, WIDE), BF16),
            pltpu.VMEM((NM, 8, WIDE), BF16),
            pltpu.VMEM((NM, 8, WIDE), F32),
            pltpu.VMEM((NM, 8, 128), F32),
            pltpu.VMEM((NY, 8, WIDE), F32),
            pltpu.VMEM((NM, 8, 128), F32),
            pltpu.VMEM((NY, 8, 256), F32),
            pltpu.VMEM((NY, 8, 256), F32),
            table, table, table, table, table, table,
            pltpu.VMEM((128, 128), BF16),
            pltpu.VMEM((32, 256), F32),
            pltpu.VMEM((32, 256), BF16),
            table,
            pltpu.VMEM((NY, 8, 128), F32),
            pltpu.VMEM((144, 256), F32),
            pltpu.VMEM((NM, 8, 256), BF16),
            pltpu.VMEM((NM, 8, 256), BF16),
            state,
            state, state, state, state, state, state, state,
            pltpu.VMEM((2, NZ, 40, 128), F32),
            pltpu.VMEM((2, NM, 1, 128), F32),
            pltpu.VMEM((NM, 16, 256), BF16),
            pltpu.VMEM((NM, 16, 256), BF16),
            dma((7,)),
            dma((NM,)), dma((CHUNKS, NM)),
            dma((NM,)), dma((NM,)),
            dma((2, NZ)), dma((2, NZ)),
            dma((2, NM)), dma((2, NM)),
            dma((NY,)), dma((NY,)),
            dma((NM,)), dma((NM,)),
        ],
        compiler_params=pltpu.CompilerParams(
            collective_id=0, has_side_effects=True, vmem_limit_bytes=67_000_000),
        name="cg",
    )(column_count, grid_block, jt, obs_weights, departures, sqrt_cov)
    inc, res = pl.pallas_call(
        finish,
        out_shape=(jax.ShapeDtypeStruct((L, 256), F32),) * 2,
        in_specs=[vmem],
        out_specs=(vmem, vmem),
        name="order",
    )(got)
    return inc.T, res.T


def solution(mesh):
    split = Mesh(mesh.devices.reshape(NY, NZ, NX, NC), ("obs_0", "obs_1", "chan_0", "chan_1"))
    return jax.shard_map(
        per_device,
        mesh=split,
        in_specs=(P(OBS, CHAN, None), P(CHAN, OBS), P(CHAN, OBS), P(OBS), P(OBS), P()),
        out_specs=(P(OBS, None), P(OBS, None)),
        check_vma=False,
    )
```

```python
import functools

import jax
import jax.numpy as jnp
from jax import lax
from jax.experimental import pallas as pl
from jax.experimental.pallas import tpu as pltpu
from jax.sharding import Mesh
from jax.sharding import PartitionSpec as P

ITERS = 5
L = 137
NY, NZ, NX, NC = 4, 8, 4, 2
NCH = NX * NC
NM = NY * NCH
LH = 35
CHUNKS = 5
PER = LH // CHUNKS
WIDE = LH * 128
ID_LANE = 16
OBS = ("obs_0", "obs_1")
CHAN = ("chan_0", "chan_1")
MESH = pl.DeviceIdType.MESH
F32 = jnp.float32
BF16 = jnp.bfloat16


def iota(shape, dim):
    return lax.broadcasted_iota(jnp.int32, shape, dim)


def dot(a, b):
    return jnp.dot(a, b, preferred_element_type=F32)


def dot_t(a, b):
    return lax.dot_general(a, b, (((1,), (1,)), ((), ())), preferred_element_type=F32)


def halves(v):
    hi = v.astype(BF16)
    return hi, (v - hi.astype(F32)).astype(BF16)


def lanes(q):
    return pl.ds(q * 128, 128)


def kernel(
    cnt_hbm, gb_hbm, jt_hbm, w_hbm, d_hbm, s_hbm,
    got_ref,
    cnt_ref, gb_ref, jv, w_ref, d_ref, s_ref,
    sb, jr, jf, mw, fx, sv, pn, pv, sc, ff, sh, sl, qh, ql, perm, eye, spot, own, near, pick, ids, tt, so, sr, cm,
    r, p, s, x, w, v, g, mz, sx, out, got,
    fs, js, jq, as_, aq, zs, zq, xs, xq, ys, yq, os, oq,
):
    my_y = lax.axis_index("obs_0")
    my_z = lax.axis_index("obs_1")
    my_x = lax.axis_index("chan_0")
    my_c = lax.axis_index("chan_1")
    my_m = my_y * NCH + my_x * NC + my_c

    fetches = [
        pltpu.make_async_copy(a, b, fs.at[k])
        for k, (a, b) in enumerate((
            (w_hbm, w_ref), (d_hbm, d_ref), (cnt_hbm, cnt_ref), (gb_hbm, gb_ref), (s_hbm, s_ref)))
    ]
    blocks = [
        pltpu.make_async_copy(jt_hbm.at[first:last], jv.at[first:last], fs.at[len(fetches) + q])
        for q, (first, last) in enumerate(((0, 4 * PER), (4 * PER, L)))
    ]
    for copy in (blocks[0], *fetches, *blocks[1:]):
        copy.start()

    def plane_peer(m):
        return (m >> 3, my_z, (m >> 1) & 3, m & 1)

    def ahead_by(t):
        return (((my_y + (t >> 2)) & 3) << 3) + (((my_x + t) & 3) << 1) + ((my_c + (t >> 4)) & 1)

    def behind_by(t):
        return (((my_y - (t >> 2)) & 3) << 3) + (((my_x - t) & 3) << 1) + ((my_c + (t >> 4)) & 1)

    def ring_peer(z):
        return (my_y, z, my_x, my_c)

    barrier = pltpu.get_barrier_semaphore()

    def greet_plane(t, carry):
        pl.semaphore_signal(barrier, inc=1, device_id=plane_peer((my_m + t) & 31), device_id_type=MESH)
        return carry

    def greet_ring(t, carry):
        pl.semaphore_signal(barrier, inc=1, device_id=ring_peer((my_z + t) & 7), device_id_type=MESH)
        return carry

    lax.fori_loop(1, NM, greet_plane, 0)
    lax.fori_loop(1, NZ, greet_ring, 0)

    row = iota((256, 256), 0)
    col = iota((256, 256), 1)
    lane = iota((8, 128), 1)
    lane1 = iota((1, 128), 1)
    perm[...] = jnp.where(
        ((row & 4) << 5) + ((row >> 3) << 2) + (row & 3) == col, 1.0, 0.0).astype(BF16)
    jv[L:144] = jnp.zeros((144 - L, 32, 256), BF16)

    def turn(h, carry):
        block = jv[pl.ds(4 * h, 4)].reshape(128, 256)
        turned = dot_t(perm[...], block).astype(BF16)
        sb[:, :, pl.ds(pl.multiple_of(h * 128, 128), 128)] = turned.reshape(NM, 8, 128)
        return carry

    def chunk(q):
        return pl.ds(q * PER * 128, PER * 128)

    def send_chunk(q):
        def send(t, carry):
            m = ahead_by(t)
            pltpu.make_async_remote_copy(
                src_ref=sb.at[m, :, chunk(q)], dst_ref=jr.at[my_m, :, chunk(q)],
                send_sem=js.at[m], recv_sem=jq.at[q, my_m],
                device_id=plane_peer(m), device_id_type=MESH).start()
            return carry

        lax.fori_loop(1, NM, send, 0)

    def chunk_wait(q, m):
        pltpu.make_async_remote_copy(
            src_ref=sb.at[m, :, chunk(q)], dst_ref=jr.at[m, :, chunk(q)],
            send_sem=js.at[m], recv_sem=jq.at[q, m],
            device_id=plane_peer(m), device_id_type=MESH).wait_recv()

    blocks[0].wait()
    lax.fori_loop(0, PER, turn, 0, unroll=True)
    pl.semaphore_wait(barrier, NM - 1 + NZ - 1)
    send_chunk(0)

    for copy in fetches:
        copy.wait()
    sh[...] = jnp.zeros_like(sh)
    sl[...] = jnp.zeros_like(sl)
    root_hi, root_lo = halves(s_ref[...])
    sh[0:L, 0:L] = root_hi
    sl[0:L, 0:L] = root_lo
    r4 = iota((8, 128), 0)
    ids[my_y] = jnp.where(r4 < 4, gb_ref[0], gb_ref[1]).astype(F32)

    def id_copy(t, arriving):
        peer = (my_y + t) & 3
        at = peer if arriving else my_y
        return pltpu.make_async_remote_copy(
            src_ref=ids.at[at], dst_ref=ids.at[at], send_sem=ys.at[t], recv_sem=yq.at[at],
            device_id=(peer, my_z, my_x, my_c), device_id_type=MESH)

    for t in range(1, NY):
        id_copy(t, False).start()

    mask = jnp.where(iota((32, 256), 1) < cnt_ref[0], 1.0, 0.0)
    weight = mask * w_ref[...]
    weight_hi, weight_lo = halves(weight)
    scaled_d = (weight * d_ref[...]).astype(BF16)
    d_ref[...] = scaled_d.astype(F32)

    for copy in blocks[1:]:
        copy.wait()

    def gather_source(g, carry):
        part = jv[pl.ds(8 * g, 8)].astype(F32) * d_ref[...][None]
        tt[pl.ds(pl.multiple_of(8 * g, 8), 8), :] = jnp.sum(part, axis=1)
        return carry

    lax.fori_loop(0, 18, gather_source, 0, unroll=2)
    hi, lo = halves(tt[...])
    flat = dot_t(perm[...], hi) + dot_t(perm[...], lo)
    so[...] = jnp.pad(flat, ((0, 0), (0, 112))).astype(BF16).reshape(NM, 8, 256)

    def source_send(t, carry):
        m = (my_m + t) & 31
        pltpu.make_async_remote_copy(
            src_ref=so.at[m], dst_ref=sr.at[my_m], send_sem=as_.at[0], recv_sem=aq.at[0],
            device_id=plane_peer(m), device_id_type=MESH).start()
        return carry

    lax.fori_loop(1, NM, source_send, 0, unroll=True)
    sr[my_m] = so[my_m]

    for q in range(1, CHUNKS):
        if q < CHUNKS - 1:
            lax.fori_loop(q * PER, (q + 1) * PER, turn, 0, unroll=True)
        else:
            lax.fori_loop(q * PER, LH - 1, turn, 0, unroll=True)
            block = jnp.concatenate([jv[L - 1], weight_hi, weight_lo, jnp.zeros_like(weight_hi)], axis=0)
            sb[:, :, lanes(LH - 1)] = dot_t(perm[...], block).astype(BF16).reshape(NM, 8, 128)
        send_chunk(q)
    jr[my_m] = sb[my_m]

    eye[...] = jnp.where(row == col, 1.0, 0.0).astype(BF16)
    spot[...] = jnp.where(
        iota((128, 128), 0) >> 5 == (iota((128, 128), 1) & 3), 1.0, 0.0).astype(BF16)
    turned_hi = dot_t(eye[...], sh[...]).astype(BF16)
    turned_lo = dot_t(eye[...], sl[...]).astype(BF16)
    square = dot(turned_hi, sh[...]) + dot(turned_lo, sh[...]) + dot(turned_hi, sl[...])
    qh[...], ql[...] = halves(square)
    for t in range(1, NY):
        id_copy(t, True).wait()
    row2 = iota((8, 256), 0)
    lane2 = iota((8, 256), 1)
    for y in range(NY):
        ident = ids[y][:, 0:1].astype(jnp.int32)
        own[pl.ds(8 * y, 8), :] = jnp.where(
            (ident == lane2 >> 2) & ((row2 & 3) == (lane2 & 3)), 1.0, 0.0)

    def source_wait():
        pltpu.make_async_remote_copy(
            src_ref=so.at[pl.ds(0, NM - 1)], dst_ref=sr.at[pl.ds(0, NM - 1)],
            send_sem=as_.at[0], recv_sem=aq.at[0],
            device_id=plane_peer(my_m ^ 1), device_id_type=MESH).wait()

    def ring_copy(slot, t, arriving):
        z = (my_z + t) & 7
        at = z if arriving else my_z
        return pltpu.make_async_remote_copy(
            src_ref=mz.at[slot, at], dst_ref=mz.at[slot, at],
            send_sem=zs.at[slot, t], recv_sem=zq.at[slot, at],
            device_id=ring_peer(z), device_id_type=MESH)

    def ring_start(slot, part):
        for t in (4, 3, 5, 2, 6, 1, 7):
            pltpu.make_async_remote_copy(
                src_ref=mz.at[slot, my_z, part], dst_ref=mz.at[slot, my_z, part],
                send_sem=zs.at[slot, t], recv_sem=zq.at[slot, my_z],
                device_id=ring_peer((my_z + t) & 7), device_id_type=MESH).start()

    def ring_tail(slot, tails):
        packed = None
        for y in range(NY):
            part = jnp.where(lane == ID_LANE, ids[y], tails[y])
            part = pltpu.roll(part, 32 * y, 1) if y else part
            packed = part if packed is None else packed + part
        mz[slot, my_z, 32:40] = packed
        ring_start(slot, pl.ds(32, 8))

    def ring_wait(slot):
        for t in range(1, NZ):
            ring_copy(slot, t, True).wait()
        for z in range(NZ):
            cm[32 * z: 32 * z + 32, 0:128] = mz[slot, z, 0:32]
            packed = mz[slot, z, 32:40]
            for y in range(NY):
                at = 32 * z + 8 * y
                cm[at: at + 8, 128:256] = pltpu.roll(packed, 128 - 32 * y, 1) if y else packed

    def times(a, hi_ref, lo_ref):
        hi, lo = halves(a)
        return dot(hi, hi_ref[...]) + dot(lo, hi_ref[...]) + dot(hi, lo_ref[...])

    def near_field():
        hi, lo = halves(cm[...])
        return times(dot(near[...], hi) + dot(near[...], lo), qh, ql).reshape(NY, 8, 256)

    def collected():
        hi, lo = halves(cm[...])
        hi, lo = halves(dot(pick[...], hi) + dot(pick[...], lo))
        return dot_t(hi, sh[...]) + dot_t(lo, sh[...]) + dot_t(hi, sl[...])

    def across(a):
        a = a + pltpu.roll(a, 64, 1)
        return a + pltpu.roll(a, 32, 1)

    def convert(q, m):
        tile = jr[m, :, chunk(q)].astype(F32)
        if q == CHUNKS - 1:
            extra = tile[:, (PER - 1) * 128:]
            mw[m] = across(jnp.where((lane >= 32) & (lane < 96), extra, 0.0))
            tile = jnp.concatenate([tile[:, : (PER - 1) * 128], jnp.where(lane < 32, extra, 0.0)], axis=1)
        jf[m, :, chunk(q)] = tile
        return tile

    def predict_part(q, m, tile):
        wide = tile * fx[m >> 3, :, chunk(q)]
        total = wide[:, 0:128]
        for h in range(1, PER):
            total = total + wide[:, 128 * h: 128 * h + 128]
        sv[m] = total if q == 0 else sv[m] + total

    def every_piece(q, work, waits):
        def pair(t, carry):
            m = behind_by(2 * t)
            n = behind_by(2 * t + 1)
            if waits:
                chunk_wait(q, m)
                chunk_wait(q, n)
            work(m)
            work(n)
            return carry

        first = behind_by(1)
        if waits:
            chunk_wait(q, first)
        work(my_m)
        work(first)
        lax.fori_loop(1, NM // 2, pair, 0)

    every_piece(0, functools.partial(convert, 0), True)
    source_wait()
    arrived = jnp.sum(sr[...].astype(F32).reshape(NY, NCH, 8, 256), axis=1)
    mz[0, my_z, 0:32] = arrived[:, :, 0:128].reshape(32, 128)
    ring_start(0, pl.ds(0, 32))
    ring_tail(0, arrived[:, :, 128:256])
    every_piece(1, functools.partial(convert, 1), True)
    ring_wait(0)
    ident = cm[:, 128 + ID_LANE: 128 + ID_LANE + 1].astype(jnp.int32)
    match = jnp.where((ident == col >> 2) & ((row & 3) == (col & 3)), 1.0, 0.0).astype(BF16)
    pick[...] = dot_t(eye[...], match).astype(BF16)
    near[...] = dot_t(own[...].astype(BF16), match).astype(BF16)
    ff[...] = near_field()
    r[...] = collected()

    def widen(y):
        for h in range(LH):
            base = ff[y, :, 0:128] if h < 32 else ff[y, :, 128:256]
            fx[y, :, lanes(h)] = jnp.take_along_axis(base, 4 * (h % 32) + (lane >> 5), axis=1)

    def group_terms(slot, y, factors):
        acc = []
        for h in range(LH):
            total = None
            for c in range(NCH):
                prod = jf[y * NCH + c, :, lanes(h)] * factors[c]
                total = prod if total is None else total + prod
            acc.append(total)
        hi, lo = halves(jnp.concatenate(acc, axis=0))
        sums = dot(hi, spot[...]) + dot(lo, spot[...])
        first = jnp.zeros((8, 128), F32)
        second = jnp.zeros((8, 128), F32)
        for h in range(LH):
            piece = jnp.where(lane >> 2 == h % 32, sums[8 * h: 8 * h + 8], 0.0)
            if h < 32:
                first = first + piece
            else:
                second = second + piece
        part = pl.ds(pl.multiple_of(8 * y, 8), 8)
        mz[slot, my_z, part] = first
        g[part, 0:128] = second
        ring_start(slot, part)

    def send_tail(slot):
        ring_tail(slot, [g[8 * y: 8 * y + 8, 0:128] for y in range(NY)])

    def widen_group(y, carry):
        widen(y)
        return carry

    lax.fori_loop(0, NY, widen_group, 0)

    for q in (0, 1):
        every_piece(q, lambda m: predict_part(q, m, jf[m, :, chunk(q)]), False)
    for q in range(2, CHUNKS):
        every_piece(q, lambda m: predict_part(q, m, convert(q, m)), True)

    def sent(t, carry):
        m = (my_m + t) & 31
        pltpu.make_async_remote_copy(
            src_ref=sb.at[m], dst_ref=jr.at[m], send_sem=js.at[m], recv_sem=jq.at[0, m],
            device_id=plane_peer(m), device_id_type=MESH).wait_send()
        return carry

    def first_group(y, carry):
        for c in range(NCH):
            sv[y * NCH + c] = across(sv[y * NCH + c])
        group_terms(1, y, [mw[y * NCH + c] * sv[y * NCH + c] for c in range(NCH)])
        return carry

    lax.fori_loop(0, NY, first_group, 0)
    send_tail(1)
    lax.fori_loop(1, NM, sent, 0)
    p[...] = jnp.zeros_like(p)
    s[...] = jnp.zeros_like(s)
    x[...] = jnp.zeros_like(x)
    v[...] = jnp.zeros_like(v)
    pv[...] = jnp.zeros_like(pv)
    sc[...] = jnp.where(iota((8, 128), 0) == 0, -1.0, 0.0)

    def plane_start(slot, t):
        pltpu.make_async_remote_copy(
            src_ref=sx.at[slot, my_m], dst_ref=sx.at[slot, my_m],
            send_sem=xs.at[slot], recv_sem=xq.at[slot],
            device_id=plane_peer((my_m + t) & 31), device_id_type=MESH).start()

    def plane_wait(slot):
        most = sx.at[slot, pl.ds(0, NM - 1)]
        pltpu.make_async_remote_copy(
            src_ref=most, dst_ref=most, send_sem=xs.at[slot], recv_sem=xq.at[slot],
            device_id=plane_peer(my_m ^ 1), device_id_type=MESH).wait()

    def scalars_send(slot):
        res = r[...]
        norm = jnp.sum(res * res, axis=0, keepdims=True)
        norm = norm[:, 0:128] + norm[:, 128:256]
        bend = jnp.sum(res * w[...], axis=0, keepdims=True)
        bend = bend[:, 0:128] + bend[:, 128:256]
        sx[slot, my_m] = jnp.where(
            lane1 < 64, norm + pltpu.roll(norm, 64, 1), bend + pltpu.roll(bend, 64, 1))

        for t in range(1, NM):
            plane_start(slot, t)

    def scalars_keep(i):
        slot = i & 1
        step_old, norm_old = sc[0:1, 0:1], sc[2:3, 0:1]

        plane_wait(slot)
        both = jnp.sum(sx[slot], axis=0)
        norm = jnp.sum(jnp.where(lane1 < 64, both, 0.0), axis=1, keepdims=True)
        bend = jnp.sum(jnp.where(lane1 < 64, 0.0, both), axis=1, keepdims=True)
        ratio = jnp.where(i == 0, 0.0, norm / norm_old)
        step = norm / (bend - jnp.where(i == 0, 0.0, ratio * norm / step_old))
        place = iota((8, 128), 0)
        sc[...] = jnp.where(place == 0, step, jnp.where(place == 1, ratio, norm))

    def catch_up(i, step, ratio):
        more = collected()

        @pl.when(i == 0)
        def start_w():
            w[...] = r[...] + more

        @pl.when(i > 0)
        def move():
            old = w[...]
            turned = old + ratio * s[...]
            s[...] = turned
            ahead = r[...] + ratio * p[...]
            p[...] = ahead
            x[...] = x[...] + step * ahead
            r[...] = r[...] - step * turned
            along = old + more + ratio * v[...]
            v[...] = along
            w[...] = old - step * along

        scalars_send(i & 1)

    def iteration(i, carry):
        ring_wait((i + 1) & 1)
        ff[...] = near_field()

        def predict(y, carry):
            widen(y)
            totals = [None] * NCH
            for h in range(LH):
                wide = fx[y, :, lanes(h)]
                for c in range(NCH):
                    prod = jf[y * NCH + c, :, lanes(h)] * wide
                    totals[c] = prod if totals[c] is None else totals[c] + prod
            for c in range(NCH):
                pn[y * NCH + c] = across(totals[c])
            return carry

        lax.fori_loop(0, NY, predict, 0)

        @pl.when(i > 0)
        def scalars():
            scalars_keep(i - 1)

        step, ratio = sc[0:1, 0:1], sc[1:2, 0:1]
        begun = jnp.where(i > 0, 1.0, 0.0)

        def group(y, carry):
            factors = []
            for c in range(NCH):
                m = y * NCH + c
                old = sv[m]
                along = begun * old + pn[m] + ratio * pv[m]
                pv[m] = along
                new = old - step * along
                sv[m] = new
                factors.append(mw[m] * new)
            group_terms(i & 1, y, factors)
            return carry

        lax.fori_loop(0, NY, group, 0)
        send_tail(i & 1)
        catch_up(i, step, ratio)
        return carry

    lax.fori_loop(0, ITERS - 1, iteration, 0)
    last = ITERS - 1
    ring_wait(last + 1 & 1)
    scalars_keep(last - 1)
    catch_up(last, sc[0:1, 0:1], sc[1:2, 0:1])
    cm[...] = times(r[...], sh, sl)
    v[...] = times(p[...], sh, sl)
    g[...] = times(x[...], sh, sl)
    scalars_keep(last)
    step, ratio = sc[0:1, 0:1], sc[1:2, 0:1]
    grown = g[...] + step * (cm[...] + ratio * v[...])
    left = r[...] - step * (w[...] + ratio * s[...])
    out[:, 0:8, :] = grown.astype(BF16).reshape(NM, 8, 256)
    out[:, 8:16, :] = left.astype(BF16).reshape(NM, 8, 256)

    def give(t, carry):
        m = (my_m + t) & 31
        pltpu.make_async_remote_copy(
            src_ref=out.at[((m >> 3) << 3) + my_z], dst_ref=got.at[my_m],
            send_sem=os.at[0], recv_sem=oq.at[0],
            device_id=plane_peer(m), device_id_type=MESH).start()
        return carry

    lax.fori_loop(1, NM, give, 0, unroll=True)
    got[my_m] = out[my_y * NZ + my_z]
    pltpu.make_async_remote_copy(
        src_ref=out.at[pl.ds(0, NM - 1)], dst_ref=got.at[pl.ds(0, NM - 1)],
        send_sem=os.at[0], recv_sem=oq.at[0],
        device_id=plane_peer(my_m ^ 1), device_id_type=MESH).wait()
    got_ref[...] = got[...]


def finish(got_ref, inc_ref, res_ref):
    row = iota((256, 256), 0)
    col = iota((256, 256), 1)
    order = jnp.where(
        ((row & 4) << 5) + ((row >> 3) << 2) + (row & 3) == col, 1.0, 0.0).astype(BF16)
    eye = jnp.where(iota((144, 256), 0) == iota((144, 256), 1), 1.0, 0.0).astype(BF16)
    for k, ref in ((0, inc_ref), (1, res_ref)):
        rows = got_ref[:, 8 * k: 8 * k + 8, :].reshape(256, 256)
        ref[...] = dot(dot_t(eye, rows).astype(BF16), order)[0:L]


def per_device(jacobian, departures, obs_weights, column_count, grid_block, sqrt_cov):
    jt = jnp.transpose(jacobian, (2, 1, 0))
    vmem = pl.BlockSpec(memory_space=pltpu.VMEM)
    dma = pltpu.SemaphoreType.DMA
    state = pltpu.VMEM((256, 256), F32)
    table = pltpu.VMEM((256, 256), BF16)
    got = pl.pallas_call(
        kernel,
        out_shape=jax.ShapeDtypeStruct((NM, 16, 256), BF16),
        in_specs=[pl.BlockSpec(memory_space=pltpu.HBM)] * 6,
        out_specs=vmem,
        scratch_shapes=[
            pltpu.SMEM((1,), jnp.int32),
            pltpu.SMEM((2,), jnp.int32),
            pltpu.VMEM((144, 32, 256), BF16),
            pltpu.VMEM((32, 256), F32),
            pltpu.VMEM((32, 256), F32),
            pltpu.VMEM((L, L), F32),
            pltpu.VMEM((NM, 8, WIDE), BF16),
            pltpu.VMEM((NM, 8, WIDE), BF16),
            pltpu.VMEM((NM, 8, WIDE), F32),
            pltpu.VMEM((NM, 8, 128), F32),
            pltpu.VMEM((NY, 8, WIDE), F32),
            pltpu.VMEM((NM, 8, 128), F32),
            pltpu.VMEM((NM, 8, 128), F32),
            pltpu.VMEM((NM, 8, 128), F32),
            pltpu.VMEM((8, 128), F32),
            pltpu.VMEM((NY, 8, 256), F32),
            table, table, table, table, table, table,
            pltpu.VMEM((128, 128), BF16),
            pltpu.VMEM((32, 256), F32),
            pltpu.VMEM((32, 256), BF16),
            table,
            pltpu.VMEM((NY, 8, 128), F32),
            pltpu.VMEM((144, 256), F32),
            pltpu.VMEM((NM, 8, 256), BF16),
            pltpu.VMEM((NM, 8, 256), BF16),
            state,
            state, state, state, state, state, state, state,
            pltpu.VMEM((2, NZ, 40, 128), F32),
            pltpu.VMEM((2, NM, 1, 128), F32),
            pltpu.VMEM((NM, 16, 256), BF16),
            pltpu.VMEM((NM, 16, 256), BF16),
            dma((7,)),
            dma((NM,)), dma((CHUNKS, NM)),
            dma((1,)), dma((1,)),
            dma((2, NZ)), dma((2, NZ)),
            dma((2,)), dma((2,)),
            dma((NY,)), dma((NY,)),
            dma((1,)), dma((1,)),
        ],
        compiler_params=pltpu.CompilerParams(
            collective_id=0, has_side_effects=True, vmem_limit_bytes=67_000_000),
        name="cg",
    )(column_count, grid_block, jt, obs_weights, departures, sqrt_cov)
    inc, res = pl.pallas_call(
        finish,
        out_shape=(jax.ShapeDtypeStruct((L, 256), F32),) * 2,
        in_specs=[vmem],
        out_specs=(vmem, vmem),
        name="order",
    )(got)
    return inc.T, res.T


def solution(mesh):
    split = Mesh(mesh.devices.reshape(NY, NZ, NX, NC), ("obs_0", "obs_1", "chan_0", "chan_1"))
    return jax.shard_map(
        per_device,
        mesh=split,
        in_specs=(P(OBS, CHAN, None), P(CHAN, OBS), P(CHAN, OBS), P(OBS), P(OBS), P()),
        out_specs=(P(OBS, None), P(OBS, None)),
        check_vma=False,
    )
```

```python
import functools

import jax
import jax.numpy as jnp
from jax import lax
from jax.experimental import pallas as pl
from jax.experimental.pallas import tpu as pltpu
from jax.sharding import Mesh
from jax.sharding import PartitionSpec as P

ITERS = 5
L = 137
NY, NZ, NX, NC = 4, 8, 4, 2
NCH = NX * NC
NM = NY * NCH
LH = 35
CHUNKS = 7
PER = LH // CHUNKS
WIDE = LH * 128
ID_LANE = 16
OBS = ("obs_0", "obs_1")
CHAN = ("chan_0", "chan_1")
MESH = pl.DeviceIdType.MESH
F32 = jnp.float32
BF16 = jnp.bfloat16


def iota(shape, dim):
    return lax.broadcasted_iota(jnp.int32, shape, dim)


def dot(a, b):
    return jnp.dot(a, b, preferred_element_type=F32)


def dot_t(a, b):
    return lax.dot_general(a, b, (((1,), (1,)), ((), ())), preferred_element_type=F32)


def halves(v):
    hi = v.astype(BF16)
    return hi, (v - hi.astype(F32)).astype(BF16)


def lanes(q):
    return pl.ds(q * 128, 128)


def kernel(
    cnt_hbm, gb_hbm, jt_hbm, w_hbm, d_hbm, s_hbm,
    got_ref,
    cnt_ref, gb_ref, jv, w_ref, d_ref, s_ref,
    sb, jr, jf, mw, fx, sv, pn, pv, sc, ff, sh, sl, qh, ql, perm, eye, spot, own, near, pick, ids, tt, so, sr, cm,
    r, p, s, x, w, v, g, mz, sx, out, got,
    fs, js, jq, as_, aq, zs, zq, xs, xq, ys, yq, os, oq,
):
    my_y = lax.axis_index("obs_0")
    my_z = lax.axis_index("obs_1")
    my_x = lax.axis_index("chan_0")
    my_c = lax.axis_index("chan_1")
    my_m = my_y * NCH + my_x * NC + my_c

    fetches = [
        pltpu.make_async_copy(a, b, fs.at[k])
        for k, (a, b) in enumerate((
            (w_hbm, w_ref), (d_hbm, d_ref), (cnt_hbm, cnt_ref), (gb_hbm, gb_ref), (s_hbm, s_ref)))
    ]
    blocks = [
        pltpu.make_async_copy(jt_hbm.at[first:last], jv.at[first:last], fs.at[len(fetches) + q])
        for q, (first, last) in enumerate(((0, 4 * PER), (4 * PER, L)))
    ]
    for copy in (blocks[0], *fetches, *blocks[1:]):
        copy.start()

    def plane_peer(m):
        return (m >> 3, my_z, (m >> 1) & 3, m & 1)

    def ahead_by(t):
        return (((my_y + (t >> 2)) & 3) << 3) + (((my_x + t) & 3) << 1) + ((my_c + (t >> 4)) & 1)

    def behind_by(t):
        return (((my_y - (t >> 2)) & 3) << 3) + (((my_x - t) & 3) << 1) + ((my_c + (t >> 4)) & 1)

    def ring_peer(z):
        return (my_y, z, my_x, my_c)

    barrier = pltpu.get_barrier_semaphore()

    def greet_plane(t, carry):
        pl.semaphore_signal(barrier, inc=1, device_id=plane_peer((my_m + t) & 31), device_id_type=MESH)
        return carry

    def greet_ring(t, carry):
        pl.semaphore_signal(barrier, inc=1, device_id=ring_peer((my_z + t) & 7), device_id_type=MESH)
        return carry

    lax.fori_loop(1, NM, greet_plane, 0, unroll=True)
    lax.fori_loop(1, NZ, greet_ring, 0, unroll=True)

    row = iota((256, 256), 0)
    col = iota((256, 256), 1)
    lane = iota((8, 128), 1)
    lane1 = iota((1, 128), 1)
    perm[...] = jnp.where(
        ((row & 4) << 5) + ((row >> 3) << 2) + (row & 3) == col, 1.0, 0.0).astype(BF16)
    jv[L:144] = jnp.zeros((144 - L, 32, 256), BF16)

    def turn(h, carry):
        block = jv[pl.ds(4 * h, 4)].reshape(128, 256)
        turned = dot_t(perm[...], block).astype(BF16)
        sb[:, :, pl.ds(pl.multiple_of(h * 128, 128), 128)] = turned.reshape(NM, 8, 128)
        return carry

    def chunk(q):
        return pl.ds(q * PER * 128, PER * 128)

    def send_chunk(q):
        def send(t, carry):
            m = ahead_by(t)
            pltpu.make_async_remote_copy(
                src_ref=sb.at[m, :, chunk(q)], dst_ref=jr.at[my_m, :, chunk(q)],
                send_sem=js.at[0], recv_sem=jq.at[q, my_m],
                device_id=plane_peer(m), device_id_type=MESH).start()
            return carry

        lax.fori_loop(1, NM, send, 0, unroll=True)

    def chunk_wait(q, m):
        pltpu.make_async_remote_copy(
            src_ref=sb.at[m, :, chunk(q)], dst_ref=jr.at[m, :, chunk(q)],
            send_sem=js.at[0], recv_sem=jq.at[q, m],
            device_id=plane_peer(m), device_id_type=MESH).wait_recv()

    blocks[0].wait()
    lax.fori_loop(0, PER, turn, 0, unroll=True)
    pl.semaphore_wait(barrier, NM - 1 + NZ - 1)
    send_chunk(0)
    blocks[1].wait()
    lax.fori_loop(PER, 2 * PER, turn, 0, unroll=True)
    send_chunk(1)

    for copy in fetches:
        copy.wait()
    sh[...] = jnp.zeros_like(sh)
    sl[...] = jnp.zeros_like(sl)
    root_hi, root_lo = halves(s_ref[...])
    sh[0:L, 0:L] = root_hi
    sl[0:L, 0:L] = root_lo
    r4 = iota((8, 128), 0)
    ids[my_y] = jnp.where(r4 < 4, gb_ref[0], gb_ref[1]).astype(F32)

    def id_copy(t, arriving):
        peer = (my_y + t) & 3
        at = peer if arriving else my_y
        return pltpu.make_async_remote_copy(
            src_ref=ids.at[at], dst_ref=ids.at[at], send_sem=ys.at[t], recv_sem=yq.at[at],
            device_id=(peer, my_z, my_x, my_c), device_id_type=MESH)

    for t in range(1, NY):
        id_copy(t, False).start()

    mask = jnp.where(iota((32, 256), 1) < cnt_ref[0], 1.0, 0.0)
    weight = mask * w_ref[...]
    weight_hi, weight_lo = halves(weight)
    scaled_d = (weight * d_ref[...]).astype(BF16)
    d_ref[...] = scaled_d.astype(F32)


    def gather_source(g, carry):
        part = jv[pl.ds(8 * g, 8)].astype(F32) * d_ref[...][None]
        tt[pl.ds(pl.multiple_of(8 * g, 8), 8), :] = jnp.sum(part, axis=1)
        return carry

    lax.fori_loop(0, 18, gather_source, 0, unroll=2)
    hi, lo = halves(tt[...])
    flat = dot_t(perm[...], hi) + dot_t(perm[...], lo)
    so[...] = jnp.pad(flat, ((0, 0), (0, 112))).astype(BF16).reshape(NM, 8, 256)

    def source_send(t, carry):
        m = (my_m + t) & 31
        pltpu.make_async_remote_copy(
            src_ref=so.at[m], dst_ref=sr.at[my_m], send_sem=as_.at[0], recv_sem=aq.at[0],
            device_id=plane_peer(m), device_id_type=MESH).start()
        return carry

    lax.fori_loop(1, NM, source_send, 0, unroll=True)
    sr[my_m] = so[my_m]

    for q in range(2, CHUNKS):
        if q < CHUNKS - 1:
            lax.fori_loop(q * PER, (q + 1) * PER, turn, 0, unroll=True)
        else:
            lax.fori_loop(q * PER, LH - 1, turn, 0, unroll=True)
            block = jnp.concatenate([jv[L - 1], weight_hi, weight_lo, jnp.zeros_like(weight_hi)], axis=0)
            sb[:, :, lanes(LH - 1)] = dot_t(perm[...], block).astype(BF16).reshape(NM, 8, 128)
        send_chunk(q)
    jr[my_m] = sb[my_m]

    eye[...] = jnp.where(row == col, 1.0, 0.0).astype(BF16)
    spot[...] = jnp.where(
        iota((128, 128), 0) >> 5 == (iota((128, 128), 1) & 3), 1.0, 0.0).astype(BF16)
    turned_hi = dot_t(eye[...], sh[...]).astype(BF16)
    turned_lo = dot_t(eye[...], sl[...]).astype(BF16)
    square = dot(turned_hi, sh[...]) + dot(turned_lo, sh[...]) + dot(turned_hi, sl[...])
    qh[...], ql[...] = halves(square)
    for t in range(1, NY):
        id_copy(t, True).wait()
    row2 = iota((8, 256), 0)
    lane2 = iota((8, 256), 1)
    for y in range(NY):
        ident = ids[y][:, 0:1].astype(jnp.int32)
        own[pl.ds(8 * y, 8), :] = jnp.where(
            (ident == lane2 >> 2) & ((row2 & 3) == (lane2 & 3)), 1.0, 0.0)

    def source_wait():
        pltpu.make_async_remote_copy(
            src_ref=so.at[pl.ds(0, NM - 1)], dst_ref=sr.at[pl.ds(0, NM - 1)],
            send_sem=as_.at[0], recv_sem=aq.at[0],
            device_id=plane_peer(my_m ^ 1), device_id_type=MESH).wait()

    def ring_start(slot, part):
        for t in (4, 3, 5, 2, 6, 1, 7):
            pltpu.make_async_remote_copy(
                src_ref=mz.at[slot, my_z, part], dst_ref=mz.at[slot, my_z, part],
                send_sem=zs.at[slot], recv_sem=zq.at[slot],
                device_id=ring_peer((my_z + t) & 7), device_id_type=MESH).start()

    def ring_tail(slot, tails):
        packed = None
        for y in range(NY):
            part = jnp.where(lane == ID_LANE, ids[y], tails[y])
            part = pltpu.roll(part, 32 * y, 1) if y else part
            packed = part if packed is None else packed + part
        mz[slot, my_z, 32:40] = packed
        ring_start(slot, pl.ds(32, 8))

    def ring_wait(slot):
        most = mz.at[slot, pl.ds(0, NZ - 1)]
        pltpu.make_async_remote_copy(
            src_ref=most, dst_ref=most, send_sem=zs.at[slot], recv_sem=zq.at[slot],
            device_id=ring_peer((my_z + 1) & 7), device_id_type=MESH).wait()
        for z in range(NZ):
            cm[32 * z: 32 * z + 32, 0:128] = mz[slot, z, 0:32]
            packed = mz[slot, z, 32:40]
            for y in range(NY):
                at = 32 * z + 8 * y
                cm[at: at + 8, 128:256] = pltpu.roll(packed, 128 - 32 * y, 1) if y else packed

    def times(a, hi_ref, lo_ref):
        hi, lo = halves(a)
        return dot(hi, hi_ref[...]) + dot(lo, hi_ref[...]) + dot(hi, lo_ref[...])

    def near_field():
        hi, lo = halves(cm[...])
        return times(dot(near[...], hi) + dot(near[...], lo), qh, ql).reshape(NY, 8, 256)

    def collected():
        hi, lo = halves(cm[...])
        hi, lo = halves(dot(pick[...], hi) + dot(pick[...], lo))
        return dot_t(hi, sh[...]) + dot_t(lo, sh[...]) + dot_t(hi, sl[...])

    def across(a):
        a = a + pltpu.roll(a, 64, 1)
        return a + pltpu.roll(a, 32, 1)

    def convert(q, m):
        tile = jr[m, :, chunk(q)].astype(F32)
        if q == CHUNKS - 1:
            extra = tile[:, (PER - 1) * 128:]
            mw[m] = across(jnp.where((lane >= 32) & (lane < 96), extra, 0.0))
            tile = jnp.concatenate([tile[:, : (PER - 1) * 128], jnp.where(lane < 32, extra, 0.0)], axis=1)
        jf[m, :, chunk(q)] = tile
        return tile

    def predict_part(q, m, tile):
        wide = tile * fx[m >> 3, :, chunk(q)]
        total = wide[:, 0:128]
        for h in range(1, PER):
            total = total + wide[:, 128 * h: 128 * h + 128]
        sv[m] = total if q == 0 else sv[m] + total

    def every_piece(q, work, waits):
        def pair(t, carry):
            m = behind_by(2 * t)
            n = behind_by(2 * t + 1)
            if waits:
                chunk_wait(q, m)
                chunk_wait(q, n)
            work(m)
            work(n)
            return carry

        first = behind_by(1)
        if waits:
            chunk_wait(q, first)
        work(my_m)
        work(first)
        lax.fori_loop(1, NM // 2, pair, 0)

    every_piece(0, functools.partial(convert, 0), True)
    source_wait()
    arrived = jnp.sum(sr[...].astype(F32).reshape(NY, NCH, 8, 256), axis=1)
    mz[0, my_z, 0:32] = arrived[:, :, 0:128].reshape(32, 128)
    ring_start(0, pl.ds(0, 32))
    ring_tail(0, arrived[:, :, 128:256])
    every_piece(1, functools.partial(convert, 1), True)
    ring_wait(0)
    ident = cm[:, 128 + ID_LANE: 128 + ID_LANE + 1].astype(jnp.int32)
    match = jnp.where((ident == col >> 2) & ((row & 3) == (col & 3)), 1.0, 0.0).astype(BF16)
    pick[...] = dot_t(eye[...], match).astype(BF16)
    near[...] = dot_t(own[...].astype(BF16), match).astype(BF16)
    ff[...] = near_field()
    r[...] = collected()

    def widen(y):
        for h in range(LH):
            base = ff[y, :, 0:128] if h < 32 else ff[y, :, 128:256]
            fx[y, :, lanes(h)] = jnp.take_along_axis(base, 4 * (h % 32) + (lane >> 5), axis=1)

    def group_terms(slot, y, factors):
        acc = []
        for h in range(LH):
            total = None
            for c in range(NCH):
                prod = jf[y * NCH + c, :, lanes(h)] * factors[c]
                total = prod if total is None else total + prod
            acc.append(total)
        hi, lo = halves(jnp.concatenate(acc, axis=0))
        sums = dot(hi, spot[...]) + dot(lo, spot[...])
        first = jnp.zeros((8, 128), F32)
        second = jnp.zeros((8, 128), F32)
        for h in range(LH):
            piece = jnp.where(lane >> 2 == h % 32, sums[8 * h: 8 * h + 8], 0.0)
            if h < 32:
                first = first + piece
            else:
                second = second + piece
        part = pl.ds(pl.multiple_of(8 * y, 8), 8)
        mz[slot, my_z, part] = first
        g[part, 0:128] = second
        ring_start(slot, part)

    def send_tail(slot):
        ring_tail(slot, [g[8 * y: 8 * y + 8, 0:128] for y in range(NY)])

    def widen_group(y, carry):
        widen(y)
        return carry

    lax.fori_loop(0, NY, widen_group, 0)

    for q in (0, 1):
        every_piece(q, lambda m: predict_part(q, m, jf[m, :, chunk(q)]), False)
    for q in range(2, CHUNKS):
        every_piece(q, lambda m: predict_part(q, m, convert(q, m)), True)

    def first_group(y, carry):
        for c in range(NCH):
            sv[y * NCH + c] = across(sv[y * NCH + c])
        group_terms(1, y, [mw[y * NCH + c] * sv[y * NCH + c] for c in range(NCH)])
        return carry

    lax.fori_loop(0, NY, first_group, 0)
    send_tail(1)
    pltpu.make_async_remote_copy(
        src_ref=sb.at[pl.ds(0, NM - 1)], dst_ref=jr.at[pl.ds(0, NM - 1)], send_sem=js.at[0],
        recv_sem=jq.at[0, 0], device_id=plane_peer(my_m ^ 1), device_id_type=MESH).wait_send()
    p[...] = jnp.zeros_like(p)
    s[...] = jnp.zeros_like(s)
    x[...] = jnp.zeros_like(x)
    v[...] = jnp.zeros_like(v)
    pv[...] = jnp.zeros_like(pv)
    sc[...] = jnp.where(iota((8, 128), 0) == 0, -1.0, 0.0)

    def plane_start(slot, t):
        pltpu.make_async_remote_copy(
            src_ref=sx.at[slot, my_m], dst_ref=sx.at[slot, my_m],
            send_sem=xs.at[slot], recv_sem=xq.at[slot],
            device_id=plane_peer((my_m + t) & 31), device_id_type=MESH).start()

    def plane_wait(slot):
        most = sx.at[slot, pl.ds(0, NM - 1)]
        pltpu.make_async_remote_copy(
            src_ref=most, dst_ref=most, send_sem=xs.at[slot], recv_sem=xq.at[slot],
            device_id=plane_peer(my_m ^ 1), device_id_type=MESH).wait()

    def scalars_send(slot):
        res = r[...]
        norm = jnp.sum(res * res, axis=0, keepdims=True)
        norm = norm[:, 0:128] + norm[:, 128:256]
        bend = jnp.sum(res * w[...], axis=0, keepdims=True)
        bend = bend[:, 0:128] + bend[:, 128:256]
        sx[slot, my_m] = jnp.where(
            lane1 < 64, norm + pltpu.roll(norm, 64, 1), bend + pltpu.roll(bend, 64, 1))

        for t in range(1, NM):
            plane_start(slot, t)

    def scalars_keep(i):
        slot = i & 1
        step_old, norm_old = sc[0:1, 0:1], sc[2:3, 0:1]

        plane_wait(slot)
        both = jnp.sum(sx[slot], axis=0)
        norm = jnp.sum(jnp.where(lane1 < 64, both, 0.0), axis=1, keepdims=True)
        bend = jnp.sum(jnp.where(lane1 < 64, 0.0, both), axis=1, keepdims=True)
        ratio = jnp.where(i == 0, 0.0, norm / norm_old)
        step = norm / (bend - jnp.where(i == 0, 0.0, ratio * norm / step_old))
        place = iota((8, 128), 0)
        sc[...] = jnp.where(place == 0, step, jnp.where(place == 1, ratio, norm))

    def catch_up(i, step, ratio):
        more = collected()

        @pl.when(i == 0)
        def start_w():
            w[...] = r[...] + more

        @pl.when(i > 0)
        def move():
            old = w[...]
            turned = old + ratio * s[...]
            s[...] = turned
            ahead = r[...] + ratio * p[...]
            p[...] = ahead
            x[...] = x[...] + step * ahead
            r[...] = r[...] - step * turned
            along = old + more + ratio * v[...]
            v[...] = along
            w[...] = old - step * along

        scalars_send(i & 1)

    def iteration(i, carry):
        ring_wait((i + 1) & 1)
        ff[...] = near_field()

        def predict(y, carry):
            widen(y)
            totals = [None] * NCH
            for h in range(LH):
                wide = fx[y, :, lanes(h)]
                for c in range(NCH):
                    prod = jf[y * NCH + c, :, lanes(h)] * wide
                    totals[c] = prod if totals[c] is None else totals[c] + prod
            for c in range(NCH):
                pn[y * NCH + c] = across(totals[c])
            return carry

        lax.fori_loop(0, NY, predict, 0)

        @pl.when(i > 0)
        def scalars():
            scalars_keep(i - 1)

        step, ratio = sc[0:1, 0:1], sc[1:2, 0:1]
        begun = jnp.where(i > 0, 1.0, 0.0)

        def group(y, carry):
            factors = []
            for c in range(NCH):
                m = y * NCH + c
                old = sv[m]
                along = begun * old + pn[m] + ratio * pv[m]
                pv[m] = along
                new = old - step * along
                sv[m] = new
                factors.append(mw[m] * new)
            group_terms(i & 1, y, factors)
            return carry

        lax.fori_loop(0, NY, group, 0)
        send_tail(i & 1)
        catch_up(i, step, ratio)
        return carry

    lax.fori_loop(0, ITERS - 1, iteration, 0)
    last = ITERS - 1
    ring_wait(last + 1 & 1)
    scalars_keep(last - 1)
    catch_up(last, sc[0:1, 0:1], sc[1:2, 0:1])
    cm[...] = times(r[...], sh, sl)
    v[...] = times(p[...], sh, sl)
    g[...] = times(x[...], sh, sl)
    scalars_keep(last)
    step, ratio = sc[0:1, 0:1], sc[1:2, 0:1]
    grown = g[...] + step * (cm[...] + ratio * v[...])
    left = r[...] - step * (w[...] + ratio * s[...])
    out[:, 0:8, :] = grown.astype(BF16).reshape(NM, 8, 256)
    out[:, 8:16, :] = left.astype(BF16).reshape(NM, 8, 256)

    def give(t, carry):
        m = (my_m + t) & 31
        pltpu.make_async_remote_copy(
            src_ref=out.at[((m >> 3) << 3) + my_z], dst_ref=got.at[my_m],
            send_sem=os.at[0], recv_sem=oq.at[0],
            device_id=plane_peer(m), device_id_type=MESH).start()
        return carry

    lax.fori_loop(1, NM, give, 0, unroll=True)
    got[my_m] = out[my_y * NZ + my_z]
    pltpu.make_async_remote_copy(
        src_ref=out.at[pl.ds(0, NM - 1)], dst_ref=got.at[pl.ds(0, NM - 1)],
        send_sem=os.at[0], recv_sem=oq.at[0],
        device_id=plane_peer(my_m ^ 1), device_id_type=MESH).wait()
    got_ref[...] = got[...]


def finish(got_ref, inc_ref, res_ref):
    row = iota((256, 256), 0)
    col = iota((256, 256), 1)
    order = jnp.where(
        ((row & 4) << 5) + ((row >> 3) << 2) + (row & 3) == col, 1.0, 0.0).astype(BF16)
    eye = jnp.where(iota((144, 256), 0) == iota((144, 256), 1), 1.0, 0.0).astype(BF16)
    for k, ref in ((0, inc_ref), (1, res_ref)):
        rows = got_ref[:, 8 * k: 8 * k + 8, :].reshape(256, 256)
        ref[...] = dot(dot_t(eye, rows).astype(BF16), order)[0:L]


def per_device(jacobian, departures, obs_weights, column_count, grid_block, sqrt_cov):
    jt = jnp.transpose(jacobian, (2, 1, 0))
    vmem = pl.BlockSpec(memory_space=pltpu.VMEM)
    dma = pltpu.SemaphoreType.DMA
    state = pltpu.VMEM((256, 256), F32)
    table = pltpu.VMEM((256, 256), BF16)
    got = pl.pallas_call(
        kernel,
        out_shape=jax.ShapeDtypeStruct((NM, 16, 256), BF16),
        in_specs=[pl.BlockSpec(memory_space=pltpu.HBM)] * 6,
        out_specs=vmem,
        scratch_shapes=[
            pltpu.SMEM((1,), jnp.int32),
            pltpu.SMEM((2,), jnp.int32),
            pltpu.VMEM((144, 32, 256), BF16),
            pltpu.VMEM((32, 256), F32),
            pltpu.VMEM((32, 256), F32),
            pltpu.VMEM((L, L), F32),
            pltpu.VMEM((NM, 8, WIDE), BF16),
            pltpu.VMEM((NM, 8, WIDE), BF16),
            pltpu.VMEM((NM, 8, WIDE), F32),
            pltpu.VMEM((NM, 8, 128), F32),
            pltpu.VMEM((NY, 8, WIDE), F32),
            pltpu.VMEM((NM, 8, 128), F32),
            pltpu.VMEM((NM, 8, 128), F32),
            pltpu.VMEM((NM, 8, 128), F32),
            pltpu.VMEM((8, 128), F32),
            pltpu.VMEM((NY, 8, 256), F32),
            table, table, table, table, table, table,
            pltpu.VMEM((128, 128), BF16),
            pltpu.VMEM((32, 256), F32),
            pltpu.VMEM((32, 256), BF16),
            table,
            pltpu.VMEM((NY, 8, 128), F32),
            pltpu.VMEM((144, 256), F32),
            pltpu.VMEM((NM, 8, 256), BF16),
            pltpu.VMEM((NM, 8, 256), BF16),
            state,
            state, state, state, state, state, state, state,
            pltpu.VMEM((2, NZ, 40, 128), F32),
            pltpu.VMEM((2, NM, 1, 128), F32),
            pltpu.VMEM((NM, 16, 256), BF16),
            pltpu.VMEM((NM, 16, 256), BF16),
            dma((7,)),
            dma((1,)), dma((CHUNKS, NM)),
            dma((1,)), dma((1,)),
            dma((2,)), dma((2,)),
            dma((2,)), dma((2,)),
            dma((NY,)), dma((NY,)),
            dma((1,)), dma((1,)),
        ],
        compiler_params=pltpu.CompilerParams(
            collective_id=0, has_side_effects=True, vmem_limit_bytes=67_000_000),
        name="cg",
    )(column_count, grid_block, jt, obs_weights, departures, sqrt_cov)
    inc, res = pl.pallas_call(
        finish,
        out_shape=(jax.ShapeDtypeStruct((L, 256), F32),) * 2,
        in_specs=[vmem],
        out_specs=(vmem, vmem),
        name="order",
    )(got)
    return inc.T, res.T


def solution(mesh):
    split = Mesh(mesh.devices.reshape(NY, NZ, NX, NC), ("obs_0", "obs_1", "chan_0", "chan_1"))
    return jax.shard_map(
        per_device,
        mesh=split,
        in_specs=(P(OBS, CHAN, None), P(CHAN, OBS), P(CHAN, OBS), P(OBS), P(OBS), P()),
        out_specs=(P(OBS, None), P(OBS, None)),
        check_vma=False,
    )
```

```python
import functools

import jax
import jax.numpy as jnp
from jax import lax
from jax.experimental import pallas as pl
from jax.experimental.pallas import tpu as pltpu
from jax.sharding import Mesh
from jax.sharding import PartitionSpec as P

ITERS = 5
L = 137
NY, NZ, NX, NC = 4, 8, 4, 2
NCH = NX * NC
NM = NY * NCH
LH = 35
CHUNKS = 7
PER = LH // CHUNKS
WIDE = LH * 128
ID_LANE = 16
OBS = ("obs_0", "obs_1")
CHAN = ("chan_0", "chan_1")
MESH = pl.DeviceIdType.MESH
F32 = jnp.float32
BF16 = jnp.bfloat16


def iota(shape, dim):
    return lax.broadcasted_iota(jnp.int32, shape, dim)


def dot(a, b):
    return jnp.dot(a, b, preferred_element_type=F32)


def dot_t(a, b):
    return lax.dot_general(a, b, (((1,), (1,)), ((), ())), preferred_element_type=F32)


def halves(v):
    hi = v.astype(BF16)
    return hi, (v - hi.astype(F32)).astype(BF16)


def lanes(q):
    return pl.ds(q * 128, 128)


def kernel(
    cnt_hbm, gb_hbm, jt_hbm, w_hbm, d_hbm, s_hbm,
    got_ref,
    cnt_ref, gb_ref, jv, w_ref, d_ref, s_ref,
    sb, jr, jf, mw, fx, sv, pn, pv, sc, ff, sh, sl, qh, ql, perm, eye, spot, own, near, pick, ids, tt, so, sr, cm,
    r, p, s, x, w, v, g, mz, sx, out, got,
    fs, js, jq, as_, aq, zs, zq, xs, xq, ys, yq, os, oq,
):
    my_y = lax.axis_index("obs_0")
    my_z = lax.axis_index("obs_1")
    my_x = lax.axis_index("chan_0")
    my_c = lax.axis_index("chan_1")
    my_m = my_y * NCH + my_x * NC + my_c

    fetches = [
        pltpu.make_async_copy(a, b, fs.at[k])
        for k, (a, b) in enumerate((
            (w_hbm, w_ref), (d_hbm, d_ref), (cnt_hbm, cnt_ref), (gb_hbm, gb_ref), (s_hbm, s_ref)))
    ]
    blocks = [
        pltpu.make_async_copy(jt_hbm.at[first:last], jv.at[first:last], fs.at[len(fetches) + q])
        for q, (first, last) in enumerate(((0, 4 * PER), (4 * PER, L)))
    ]
    for copy in (blocks[0], *fetches, *blocks[1:]):
        copy.start()

    def plane_peer(m):
        return (m >> 3, my_z, (m >> 1) & 3, m & 1)

    def ahead_by(t):
        return (((my_y + (t >> 2)) & 3) << 3) + (((my_x + t) & 3) << 1) + ((my_c + (t >> 4)) & 1)

    def behind_by(t):
        return (((my_y - (t >> 2)) & 3) << 3) + (((my_x - t) & 3) << 1) + ((my_c + (t >> 4)) & 1)

    def ring_peer(z):
        return (my_y, z, my_x, my_c)

    barrier = pltpu.get_barrier_semaphore()

    def greet_plane(t, carry):
        pl.semaphore_signal(barrier, inc=1, device_id=plane_peer((my_m + t) & 31), device_id_type=MESH)
        return carry

    def greet_ring(t, carry):
        pl.semaphore_signal(barrier, inc=1, device_id=ring_peer((my_z + t) & 7), device_id_type=MESH)
        return carry

    lax.fori_loop(1, NM, greet_plane, 0, unroll=True)
    lax.fori_loop(1, NZ, greet_ring, 0, unroll=True)

    row = iota((256, 256), 0)
    col = iota((256, 256), 1)
    lane = iota((8, 128), 1)
    lane1 = iota((1, 128), 1)
    perm[...] = jnp.where(
        ((row & 4) << 5) + ((row >> 3) << 2) + (row & 3) == col, 1.0, 0.0).astype(BF16)
    jv[L:144] = jnp.zeros((144 - L, 32, 256), BF16)

    def turn(h, carry):
        block = jv[pl.ds(4 * h, 4)].reshape(128, 256)
        turned = dot_t(perm[...], block).astype(BF16)
        sb[:, :, pl.ds(pl.multiple_of(h * 128, 128), 128)] = turned.reshape(NM, 8, 128)
        return carry

    def chunk(q):
        return pl.ds(q * PER * 128, PER * 128)

    def send_chunk(q):
        def send(t, carry):
            m = ahead_by(t)
            pltpu.make_async_remote_copy(
                src_ref=sb.at[m, :, chunk(q)], dst_ref=jr.at[my_m, :, chunk(q)],
                send_sem=js.at[0], recv_sem=jq.at[q, my_m],
                device_id=plane_peer(m), device_id_type=MESH).start()
            return carry

        lax.fori_loop(1, NM, send, 0, unroll=True)

    def chunk_wait(q, m):
        pltpu.make_async_remote_copy(
            src_ref=sb.at[m, :, chunk(q)], dst_ref=jr.at[m, :, chunk(q)],
            send_sem=js.at[0], recv_sem=jq.at[q, m],
            device_id=plane_peer(m), device_id_type=MESH).wait_recv()

    blocks[0].wait()
    lax.fori_loop(0, PER, turn, 0, unroll=True)
    pl.semaphore_wait(barrier, NM - 1 + NZ - 1)
    send_chunk(0)
    blocks[1].wait()
    lax.fori_loop(PER, 2 * PER, turn, 0, unroll=True)
    send_chunk(1)

    for copy in fetches:
        copy.wait()
    sh[...] = jnp.zeros_like(sh)
    sl[...] = jnp.zeros_like(sl)
    root_hi, root_lo = halves(s_ref[...])
    sh[0:L, 0:L] = root_hi
    sl[0:L, 0:L] = root_lo
    r4 = iota((8, 128), 0)
    ids[my_y] = jnp.where(r4 < 4, gb_ref[0], gb_ref[1]).astype(F32)

    def id_copy(t, arriving):
        peer = (my_y + t) & 3
        at = peer if arriving else my_y
        return pltpu.make_async_remote_copy(
            src_ref=ids.at[at], dst_ref=ids.at[at], send_sem=ys.at[t], recv_sem=yq.at[at],
            device_id=(peer, my_z, my_x, my_c), device_id_type=MESH)

    for t in range(1, NY):
        id_copy(t, False).start()

    mask = jnp.where(iota((32, 256), 1) < cnt_ref[0], 1.0, 0.0)
    weight = mask * w_ref[...]
    weight_hi, weight_lo = halves(weight)
    scaled_d = (weight * d_ref[...]).astype(BF16)
    d_ref[...] = scaled_d.astype(F32)


    def gather_source(g, carry):
        part = jv[pl.ds(8 * g, 8)].astype(F32) * d_ref[...][None]
        tt[pl.ds(pl.multiple_of(8 * g, 8), 8), :] = jnp.sum(part, axis=1)
        return carry

    lax.fori_loop(0, 18, gather_source, 0, unroll=2)
    hi, lo = halves(tt[...])
    flat = dot_t(perm[...], hi) + dot_t(perm[...], lo)
    so[...] = jnp.pad(flat, ((0, 0), (0, 112))).astype(BF16).reshape(NM, 8, 256)

    def source_send(t, carry):
        m = (my_m + t) & 31
        pltpu.make_async_remote_copy(
            src_ref=so.at[m], dst_ref=sr.at[my_m], send_sem=as_.at[0], recv_sem=aq.at[0],
            device_id=plane_peer(m), device_id_type=MESH).start()
        return carry

    lax.fori_loop(1, NM, source_send, 0, unroll=True)
    sr[my_m] = so[my_m]

    for q in range(2, CHUNKS):
        if q < CHUNKS - 1:
            lax.fori_loop(q * PER, (q + 1) * PER, turn, 0, unroll=True)
        else:
            lax.fori_loop(q * PER, LH - 1, turn, 0, unroll=True)
            block = jnp.concatenate([jv[L - 1], weight_hi, weight_lo, jnp.zeros_like(weight_hi)], axis=0)
            sb[:, :, lanes(LH - 1)] = dot_t(perm[...], block).astype(BF16).reshape(NM, 8, 128)
        send_chunk(q)
    jr[my_m] = sb[my_m]

    eye[...] = jnp.where(row == col, 1.0, 0.0).astype(BF16)
    spot[...] = jnp.where(
        iota((128, 128), 0) >> 5 == (iota((128, 128), 1) & 3), 1.0, 0.0).astype(BF16)
    turned_hi = dot_t(eye[...], sh[...]).astype(BF16)
    turned_lo = dot_t(eye[...], sl[...]).astype(BF16)
    square = dot(turned_hi, sh[...]) + dot(turned_lo, sh[...]) + dot(turned_hi, sl[...])
    qh[...], ql[...] = halves(square)
    for t in range(1, NY):
        id_copy(t, True).wait()
    row2 = iota((8, 256), 0)
    lane2 = iota((8, 256), 1)
    for y in range(NY):
        ident = ids[y][:, 0:1].astype(jnp.int32)
        own[pl.ds(8 * y, 8), :] = jnp.where(
            (ident == lane2 >> 2) & ((row2 & 3) == (lane2 & 3)), 1.0, 0.0)

    def source_wait():
        pltpu.make_async_remote_copy(
            src_ref=so.at[pl.ds(0, NM - 1)], dst_ref=sr.at[pl.ds(0, NM - 1)],
            send_sem=as_.at[0], recv_sem=aq.at[0],
            device_id=plane_peer(my_m ^ 1), device_id_type=MESH).wait()

    def ring_start(slot, part):
        for t in (4, 3, 5, 2, 6, 1, 7):
            pltpu.make_async_remote_copy(
                src_ref=mz.at[slot, my_z, part], dst_ref=mz.at[slot, my_z, part],
                send_sem=zs.at[slot], recv_sem=zq.at[slot],
                device_id=ring_peer((my_z + t) & 7), device_id_type=MESH).start()

    def ring_tail(slot, tails):
        packed = None
        for y in range(NY):
            part = jnp.where(lane == ID_LANE, ids[y], tails[y])
            part = pltpu.roll(part, 32 * y, 1) if y else part
            packed = part if packed is None else packed + part
        mz[slot, my_z, 32:40] = packed
        ring_start(slot, pl.ds(32, 8))

    def ring_wait(slot):
        most = mz.at[slot, pl.ds(0, NZ - 1)]
        pltpu.make_async_remote_copy(
            src_ref=most, dst_ref=most, send_sem=zs.at[slot], recv_sem=zq.at[slot],
            device_id=ring_peer((my_z + 1) & 7), device_id_type=MESH).wait()
        for z in range(NZ):
            cm[32 * z: 32 * z + 32, 0:128] = mz[slot, z, 0:32]
            packed = mz[slot, z, 32:40]
            for y in range(NY):
                at = 32 * z + 8 * y
                cm[at: at + 8, 128:256] = pltpu.roll(packed, 128 - 32 * y, 1) if y else packed

    def times(a, hi_ref, lo_ref):
        hi, lo = halves(a)
        return dot(hi, hi_ref[...]) + dot(lo, hi_ref[...]) + dot(hi, lo_ref[...])

    def near_field():
        hi, lo = halves(cm[...])
        return times(dot(near[...], hi) + dot(near[...], lo), qh, ql).reshape(NY, 8, 256)

    def collected():
        hi, lo = halves(cm[...])
        hi, lo = halves(dot(pick[...], hi) + dot(pick[...], lo))
        return dot_t(hi, sh[...]) + dot_t(lo, sh[...]) + dot_t(hi, sl[...])

    def across(a):
        a = a + pltpu.roll(a, 64, 1)
        return a + pltpu.roll(a, 32, 1)

    def convert(q, m):
        tile = jr[m, :, chunk(q)].astype(F32)
        if q == CHUNKS - 1:
            extra = tile[:, (PER - 1) * 128:]
            mw[m] = across(jnp.where((lane >= 32) & (lane < 96), extra, 0.0))
            tile = jnp.concatenate([tile[:, : (PER - 1) * 128], jnp.where(lane < 32, extra, 0.0)], axis=1)
        jf[m, :, chunk(q)] = tile
        return tile

    def predict_part(q, m, tile):
        wide = tile * fx[m >> 3, :, chunk(q)]
        total = wide[:, 0:128]
        for h in range(1, PER):
            total = total + wide[:, 128 * h: 128 * h + 128]
        sv[m] = total if q == 0 else sv[m] + total

    def every_piece(q, work, waits):
        def pair(t, carry):
            m = behind_by(2 * t)
            n = behind_by(2 * t + 1)
            if waits:
                chunk_wait(q, m)
                chunk_wait(q, n)
            work(m)
            work(n)
            return carry

        first = behind_by(1)
        if waits:
            chunk_wait(q, first)
        work(my_m)
        work(first)
        lax.fori_loop(1, NM // 2, pair, 0)

    every_piece(0, functools.partial(convert, 0), True)
    source_wait()
    arrived = jnp.sum(sr[...].astype(F32).reshape(NY, NCH, 8, 256), axis=1)
    mz[0, my_z, 0:32] = arrived[:, :, 0:128].reshape(32, 128)
    ring_start(0, pl.ds(0, 32))
    ring_tail(0, arrived[:, :, 128:256])
    every_piece(1, functools.partial(convert, 1), True)
    ring_wait(0)
    ident = cm[:, 128 + ID_LANE: 128 + ID_LANE + 1].astype(jnp.int32)
    match = jnp.where((ident == col >> 2) & ((row & 3) == (col & 3)), 1.0, 0.0).astype(BF16)
    pick[...] = dot_t(eye[...], match).astype(BF16)
    near[...] = dot_t(own[...].astype(BF16), match).astype(BF16)
    ff[...] = near_field()
    r[...] = collected()

    def widen(y):
        for h in range(LH):
            base = ff[y, :, 0:128] if h < 32 else ff[y, :, 128:256]
            fx[y, :, lanes(h)] = jnp.take_along_axis(base, 4 * (h % 32) + (lane >> 5), axis=1)

    def group_terms(slot, y, factors):
        acc = []
        for h in range(LH):
            total = None
            for c in range(NCH):
                prod = jf[y * NCH + c, :, lanes(h)] * factors[c]
                total = prod if total is None else total + prod
            acc.append(total)
        hi, lo = halves(jnp.concatenate(acc, axis=0))
        sums = dot(hi, spot[...]) + dot(lo, spot[...])
        first = jnp.zeros((8, 128), F32)
        second = jnp.zeros((8, 128), F32)
        for h in range(LH):
            piece = jnp.where(lane >> 2 == h % 32, sums[8 * h: 8 * h + 8], 0.0)
            if h < 32:
                first = first + piece
            else:
                second = second + piece
        part = pl.ds(pl.multiple_of(8 * y, 8), 8)
        mz[slot, my_z, part] = first
        g[part, 0:128] = second
        ring_start(slot, part)

    def send_tail(slot):
        ring_tail(slot, [g[8 * y: 8 * y + 8, 0:128] for y in range(NY)])

    def widen_group(y, carry):
        widen(y)
        return carry

    lax.fori_loop(0, NY, widen_group, 0)

    for q in (0, 1):
        every_piece(q, lambda m: predict_part(q, m, jf[m, :, chunk(q)]), False)
    for q in range(2, CHUNKS):
        every_piece(q, lambda m: predict_part(q, m, convert(q, m)), True)

    def first_group(y, carry):
        for c in range(NCH):
            sv[y * NCH + c] = across(sv[y * NCH + c])
        group_terms(1, y, [mw[y * NCH + c] * sv[y * NCH + c] for c in range(NCH)])
        return carry

    lax.fori_loop(0, NY, first_group, 0)
    send_tail(1)
    pltpu.make_async_remote_copy(
        src_ref=sb.at[pl.ds(0, NM - 1)], dst_ref=jr.at[pl.ds(0, NM - 1)], send_sem=js.at[0],
        recv_sem=jq.at[0, 0], device_id=plane_peer(my_m ^ 1), device_id_type=MESH).wait_send()
    p[...] = jnp.zeros_like(p)
    s[...] = jnp.zeros_like(s)
    x[...] = jnp.zeros_like(x)
    v[...] = jnp.zeros_like(v)
    pv[...] = jnp.zeros_like(pv)
    sc[...] = jnp.where(iota((8, 128), 0) == 0, -1.0, 0.0)

    def plane_start(slot, t):
        pltpu.make_async_remote_copy(
            src_ref=sx.at[slot, my_m], dst_ref=sx.at[slot, my_m],
            send_sem=xs.at[slot], recv_sem=xq.at[slot],
            device_id=plane_peer((my_m + t) & 31), device_id_type=MESH).start()

    def plane_wait(slot):
        most = sx.at[slot, pl.ds(0, NM - 1)]
        pltpu.make_async_remote_copy(
            src_ref=most, dst_ref=most, send_sem=xs.at[slot], recv_sem=xq.at[slot],
            device_id=plane_peer(my_m ^ 1), device_id_type=MESH).wait()

    def scalars_send(slot):
        res = r[...]
        norm = jnp.sum(res * res, axis=0, keepdims=True)
        norm = norm[:, 0:128] + norm[:, 128:256]
        bend = jnp.sum(res * w[...], axis=0, keepdims=True)
        bend = bend[:, 0:128] + bend[:, 128:256]
        sx[slot, my_m] = jnp.where(
            lane1 < 64, norm + pltpu.roll(norm, 64, 1), bend + pltpu.roll(bend, 64, 1))

        for t in range(1, NM):
            plane_start(slot, t)

    def scalars_keep(i):
        slot = i & 1
        step_old, norm_old = sc[0:1, 0:1], sc[2:3, 0:1]

        plane_wait(slot)
        both = jnp.sum(sx[slot], axis=0)
        norm = jnp.sum(jnp.where(lane1 < 64, both, 0.0), axis=1, keepdims=True)
        bend = jnp.sum(jnp.where(lane1 < 64, 0.0, both), axis=1, keepdims=True)
        ratio = jnp.where(i == 0, 0.0, norm / norm_old)
        step = norm / (bend - jnp.where(i == 0, 0.0, ratio * norm / step_old))
        place = iota((8, 128), 0)
        sc[...] = jnp.where(place == 0, step, jnp.where(place == 1, ratio, norm))

    def catch_up(i, step, ratio):
        more = collected()

        @pl.when(i == 0)
        def start_w():
            w[...] = r[...] + more

        @pl.when(i > 0)
        def move():
            old = w[...]
            turned = old + ratio * s[...]
            s[...] = turned
            ahead = r[...] + ratio * p[...]
            p[...] = ahead
            x[...] = x[...] + step * ahead
            r[...] = r[...] - step * turned
            along = old + more + ratio * v[...]
            v[...] = along
            w[...] = old - step * along

        scalars_send(i & 1)

    def iteration(i, carry):
        ring_wait((i + 1) & 1)
        ff[...] = near_field()

        def predict(y, carry):
            totals = [None] * NCH
            field = ff[y]
            for h in range(LH):
                base = field[:, 0:128] if h < 32 else field[:, 128:256]
                wide = jnp.take_along_axis(base, 4 * (h % 32) + (lane >> 5), axis=1)
                for c in range(NCH):
                    prod = jf[y * NCH + c, :, lanes(h)] * wide
                    totals[c] = prod if totals[c] is None else totals[c] + prod
            for c in range(NCH):
                pn[y * NCH + c] = across(totals[c])
            return carry

        lax.fori_loop(0, NY, predict, 0, unroll=2)

        @pl.when(i > 0)
        def scalars():
            scalars_keep(i - 1)

        step, ratio = sc[0:1, 0:1], sc[1:2, 0:1]
        begun = jnp.where(i > 0, 1.0, 0.0)

        def group(y, carry):
            factors = []
            for c in range(NCH):
                m = y * NCH + c
                old = sv[m]
                along = begun * old + pn[m] + ratio * pv[m]
                pv[m] = along
                new = old - step * along
                sv[m] = new
                factors.append(mw[m] * new)
            group_terms(i & 1, y, factors)
            return carry

        lax.fori_loop(0, NY, group, 0, unroll=2)
        send_tail(i & 1)
        catch_up(i, step, ratio)
        return carry

    lax.fori_loop(0, ITERS - 1, iteration, 0)
    last = ITERS - 1
    ring_wait(last + 1 & 1)
    scalars_keep(last - 1)
    catch_up(last, sc[0:1, 0:1], sc[1:2, 0:1])
    cm[...] = times(r[...], sh, sl)
    v[...] = times(p[...], sh, sl)
    g[...] = times(x[...], sh, sl)
    scalars_keep(last)
    step, ratio = sc[0:1, 0:1], sc[1:2, 0:1]
    grown = g[...] + step * (cm[...] + ratio * v[...])
    left = r[...] - step * (w[...] + ratio * s[...])
    out[:, 0:8, :] = grown.astype(BF16).reshape(NM, 8, 256)
    out[:, 8:16, :] = left.astype(BF16).reshape(NM, 8, 256)

    def give(t, carry):
        m = (my_m + t) & 31
        pltpu.make_async_remote_copy(
            src_ref=out.at[((m >> 3) << 3) + my_z], dst_ref=got.at[my_m],
            send_sem=os.at[0], recv_sem=oq.at[0],
            device_id=plane_peer(m), device_id_type=MESH).start()
        return carry

    lax.fori_loop(1, NM, give, 0, unroll=True)
    got[my_m] = out[my_y * NZ + my_z]
    pltpu.make_async_remote_copy(
        src_ref=out.at[pl.ds(0, NM - 1)], dst_ref=got.at[pl.ds(0, NM - 1)],
        send_sem=os.at[0], recv_sem=oq.at[0],
        device_id=plane_peer(my_m ^ 1), device_id_type=MESH).wait()
    got_ref[...] = got[...]


def finish(got_ref, inc_ref, res_ref):
    row = iota((256, 256), 0)
    col = iota((256, 256), 1)
    order = jnp.where(
        ((row & 4) << 5) + ((row >> 3) << 2) + (row & 3) == col, 1.0, 0.0).astype(BF16)
    eye = jnp.where(iota((144, 256), 0) == iota((144, 256), 1), 1.0, 0.0).astype(BF16)
    for k, ref in ((0, inc_ref), (1, res_ref)):
        rows = got_ref[:, 8 * k: 8 * k + 8, :].reshape(256, 256)
        ref[...] = dot(dot_t(eye, rows).astype(BF16), order)[0:L]


def per_device(jacobian, departures, obs_weights, column_count, grid_block, sqrt_cov):
    jt = jnp.transpose(jacobian, (2, 1, 0))
    vmem = pl.BlockSpec(memory_space=pltpu.VMEM)
    dma = pltpu.SemaphoreType.DMA
    state = pltpu.VMEM((256, 256), F32)
    table = pltpu.VMEM((256, 256), BF16)
    got = pl.pallas_call(
        kernel,
        out_shape=jax.ShapeDtypeStruct((NM, 16, 256), BF16),
        in_specs=[pl.BlockSpec(memory_space=pltpu.HBM)] * 6,
        out_specs=vmem,
        scratch_shapes=[
            pltpu.SMEM((1,), jnp.int32),
            pltpu.SMEM((2,), jnp.int32),
            pltpu.VMEM((144, 32, 256), BF16),
            pltpu.VMEM((32, 256), F32),
            pltpu.VMEM((32, 256), F32),
            pltpu.VMEM((L, L), F32),
            pltpu.VMEM((NM, 8, WIDE), BF16),
            pltpu.VMEM((NM, 8, WIDE), BF16),
            pltpu.VMEM((NM, 8, WIDE), F32),
            pltpu.VMEM((NM, 8, 128), F32),
            pltpu.VMEM((NY, 8, WIDE), F32),
            pltpu.VMEM((NM, 8, 128), F32),
            pltpu.VMEM((NM, 8, 128), F32),
            pltpu.VMEM((NM, 8, 128), F32),
            pltpu.VMEM((8, 128), F32),
            pltpu.VMEM((NY, 8, 256), F32),
            table, table, table, table, table, table,
            pltpu.VMEM((128, 128), BF16),
            pltpu.VMEM((32, 256), F32),
            pltpu.VMEM((32, 256), BF16),
            table,
            pltpu.VMEM((NY, 8, 128), F32),
            pltpu.VMEM((144, 256), F32),
            pltpu.VMEM((NM, 8, 256), BF16),
            pltpu.VMEM((NM, 8, 256), BF16),
            state,
            state, state, state, state, state, state, state,
            pltpu.VMEM((2, NZ, 40, 128), F32),
            pltpu.VMEM((2, NM, 1, 128), F32),
            pltpu.VMEM((NM, 16, 256), BF16),
            pltpu.VMEM((NM, 16, 256), BF16),
            dma((7,)),
            dma((1,)), dma((CHUNKS, NM)),
            dma((1,)), dma((1,)),
            dma((2,)), dma((2,)),
            dma((2,)), dma((2,)),
            dma((NY,)), dma((NY,)),
            dma((1,)), dma((1,)),
        ],
        compiler_params=pltpu.CompilerParams(
            collective_id=0, has_side_effects=True, vmem_limit_bytes=67_000_000),
        name="cg",
    )(column_count, grid_block, jt, obs_weights, departures, sqrt_cov)
    inc, res = pl.pallas_call(
        finish,
        out_shape=(jax.ShapeDtypeStruct((L, 256), F32),) * 2,
        in_specs=[vmem],
        out_specs=(vmem, vmem),
        name="order",
    )(got)
    return inc.T, res.T


def solution(mesh):
    split = Mesh(mesh.devices.reshape(NY, NZ, NX, NC), ("obs_0", "obs_1", "chan_0", "chan_1"))
    return jax.shard_map(
        per_device,
        mesh=split,
        in_specs=(P(OBS, CHAN, None), P(CHAN, OBS), P(CHAN, OBS), P(OBS), P(OBS), P()),
        out_specs=(P(OBS, None), P(OBS, None)),
        check_vma=False,
    )
```
